8 devices in a mesh: dp: 1 (over z), tp: 8 (over y, x, core).
Axes of the slice: x: 2, y: 2, z: 1, core: 2. Of those that a mesh axis runs over, the one named last changes fastest.
Arguments:
- tok_hidden: bfloat16 [256, 2048], P('dp')
- seq_lens: int32 [256], P('dp')
- k_cache: bfloat16 [256, 512, 8, 64], P('dp', None, 'tp')
- v_cache: bfloat16 [256, 512, 8, 64], P('dp', None, 'tp')
- next_tok: int32 [256], P('dp')
- g_attn: bfloat16 [2048], replicated
- w_q: bfloat16 [2048, 2048], P(None, 'tp')
- b_q: bfloat16 [2048], P('tp')
- w_k: bfloat16 [2048, 512], P(None, 'tp')
- b_k: bfloat16 [512], P('tp')
- w_v: bfloat16 [2048, 512], P(None, 'tp')
- b_v: bfloat16 [512], P('tp')
- w_o: bfloat16 [2048, 2048], P('tp')
- g_mlp: bfloat16 [2048], replicated
- w_gate: bfloat16 [2048, 8192], P(None, 'tp')
- w_up: bfloat16 [2048, 8192], P(None, 'tp')
- w_down: bfloat16 [8192, 2048], P('tp')
- g_final: bfloat16 [2048], replicated
- w_head: bfloat16 [128256, 2048], P('tp')
Outputs:
- output 1: bfloat16 [256, 2048], P('dp')
- output 2: bfloat16 [256, 512, 8, 64], P('dp', None, 'tp')
- output 3: bfloat16 [256, 512, 8, 64], P('dp', None, 'tp')
- output 4: float32 [256], P('dp')
- output 5: float32 [256], P('dp')
All inputs are finite; a program needn't handle non-finite values.
Results may differ from the reference program's by a relative error of at most 0.0134547.
Values are sent between devices in bfloat16 or wider.
A program may use at most 1 GiB of HBM per device.

```python
import math
import jax
import jax.numpy as jnp
from jax import lax

BATCH = 256
LMAX = 512
D = 2048
HEADS = 32
KV_HEADS = 8
HEAD = 64
FF = 8192
VOCAB = 128256
KV_SLOTS = 8
THETA = 1000000
EPS = 1e-6
COPIES = KV_SLOTS // KV_HEADS
GROUP = HEADS // KV_SLOTS


def rms_norm(values, gain_vec):
    vals_f32 = values.astype(jnp.float32)
    inv_rms = lax.rsqrt(jnp.mean(vals_f32 * vals_f32, axis=-1, keepdims=True) + EPS)
    return (vals_f32 * inv_rms * gain_vec.astype(jnp.float32)).astype(jnp.bfloat16)


def rotary(values, positions):
    half_dim = values.shape[-1] // 2
    inv_freq = jnp.power(float(THETA), jnp.arange(half_dim, dtype=jnp.float32) * (-2.0 / values.shape[-1]))
    angles = positions.astype(jnp.float32)[:, None] * inv_freq[None, :]
    cos_part = jnp.cos(angles)[:, None, :]
    sin_part = jnp.sin(angles)[:, None, :]
    first_half = values[..., :half_dim]
    second_half = values[..., half_dim:]
    return jnp.concatenate([first_half * cos_part - second_half * sin_part, second_half * cos_part + first_half * sin_part], axis=-1)


def draw_lengths(len_key):
    exp_key, off_key, pick_key = jax.random.split(len_key, 3)
    log_max = int(math.log2(LMAX))
    exponent = jax.random.randint(exp_key, (BATCH,), 0, log_max)
    base_len = jnp.left_shift(jnp.ones((BATCH,), jnp.int32), exponent)
    offset = jax.random.randint(off_key, (BATCH,), 0, LMAX) % base_len
    longest = jax.random.randint(pick_key, (), 0, BATCH)
    return jnp.where(jnp.arange(BATCH) == longest, LMAX - 1, base_len + offset).astype(jnp.int32)


def gaussian(rand_key, arr_shape, spread):
    return jax.random.normal(rand_key, arr_shape, jnp.float32) * spread


def setup_inputs(seed: int = 0, part: int = 0) -> dict:
    shared_keys = jax.random.split(jax.random.key(seed), 16)
    part_keys = jax.random.split(jax.random.fold_in(jax.random.key(seed + 1), part), 8)
    k_scale = math.sqrt(max(math.log(LMAX / 8.0), 1.0) / 1.25)
    k_base = gaussian(part_keys[2], (BATCH, LMAX, KV_HEADS, HEAD), k_scale)
    v_base = gaussian(part_keys[3], (BATCH, LMAX, KV_HEADS, HEAD), 1.0)
    w_k = gaussian(shared_keys[3], (D, KV_HEADS, HEAD), D ** -0.5)
    b_k = gaussian(shared_keys[4], (KV_HEADS, HEAD), 0.5)
    w_v = gaussian(shared_keys[5], (D, KV_HEADS, HEAD), D ** -0.5)
    b_v = gaussian(shared_keys[6], (KV_HEADS, HEAD), 0.5)
    return {
        'tok_hidden': gaussian(part_keys[0], (BATCH, D), 1.0).astype(jnp.bfloat16),
        'seq_lens': draw_lengths(part_keys[1]),
        'k_cache': jnp.repeat(k_base, COPIES, axis=2).astype(jnp.bfloat16),
        'v_cache': jnp.repeat(v_base, COPIES, axis=2).astype(jnp.bfloat16),
        'next_tok': jax.random.randint(part_keys[4], (BATCH,), 0, VOCAB),
        'g_attn': (1.0 + gaussian(shared_keys[0], (D,), 0.2)).astype(jnp.bfloat16),
        'w_q': gaussian(shared_keys[1], (D, HEADS * HEAD), D ** -0.5).astype(jnp.bfloat16),
        'b_q': gaussian(shared_keys[2], (HEADS * HEAD,), 0.5).astype(jnp.bfloat16),
        'w_k': jnp.repeat(w_k, COPIES, axis=1).reshape(D, KV_SLOTS * HEAD).astype(jnp.bfloat16),
        'b_k': jnp.repeat(b_k, COPIES, axis=0).reshape(KV_SLOTS * HEAD).astype(jnp.bfloat16),
        'w_v': jnp.repeat(w_v, COPIES, axis=1).reshape(D, KV_SLOTS * HEAD).astype(jnp.bfloat16),
        'b_v': jnp.repeat(b_v, COPIES, axis=0).reshape(KV_SLOTS * HEAD).astype(jnp.bfloat16),
        'w_o': gaussian(shared_keys[7], (HEADS * HEAD, D), (HEADS * HEAD) ** -0.5).astype(jnp.bfloat16),
        'g_mlp': (1.0 + gaussian(shared_keys[8], (D,), 0.2)).astype(jnp.bfloat16),
        'w_gate': gaussian(shared_keys[9], (D, FF), D ** -0.5).astype(jnp.bfloat16),
        'w_up': gaussian(shared_keys[10], (D, FF), D ** -0.5).astype(jnp.bfloat16),
        'w_down': gaussian(shared_keys[11], (FF, D), FF ** -0.5).astype(jnp.bfloat16),
        'g_final': (3.0 + gaussian(shared_keys[12], (D,), 0.5)).astype(jnp.bfloat16),
        'w_head': gaussian(shared_keys[13], (VOCAB, D), D ** -0.5).astype(jnp.bfloat16),
    }


def reference(tok_hidden, seq_lens, k_cache, v_cache, next_tok, g_attn, w_q, b_q, w_k, b_k, w_v, b_v, w_o, g_mlp, w_gate, w_up, w_down, g_final, w_head):
    normed = rms_norm(tok_hidden, g_attn)
    q_proj = jnp.dot(normed, w_q, preferred_element_type=jnp.float32) + b_q.astype(jnp.float32)
    k_proj = jnp.dot(normed, w_k, preferred_element_type=jnp.float32) + b_k.astype(jnp.float32)
    v_proj = jnp.dot(normed, w_v, preferred_element_type=jnp.float32) + b_v.astype(jnp.float32)
    q_rot = rotary(q_proj.reshape(BATCH, HEADS, HEAD), seq_lens).astype(jnp.bfloat16)
    k_new = rotary(k_proj.reshape(BATCH, KV_SLOTS, HEAD), seq_lens).astype(jnp.bfloat16)
    v_new = v_proj.reshape(BATCH, KV_SLOTS, HEAD).astype(jnp.bfloat16)
    slot_ids = jnp.arange(LMAX)
    write_mask = (slot_ids[None, :] == seq_lens[:, None])[:, :, None, None]
    k_all = jnp.where(write_mask, k_new[:, None], k_cache)
    v_all = jnp.where(write_mask, v_new[:, None], v_cache)

    def one_row(row_args):
        q_row, k_row, v_row, length = row_args
        q_grp = q_row.reshape(KV_SLOTS, GROUP, HEAD).astype(jnp.float32)
        scores = jnp.einsum('kgd,lkd->kgl', q_grp, k_row.astype(jnp.float32)) * (HEAD ** -0.5)
        scores = jnp.where((slot_ids <= length)[None, None, :], scores, -jnp.inf)
        attn_probs = jax.nn.softmax(scores, axis=-1).astype(jnp.bfloat16).astype(jnp.float32)
        attn_vals = jnp.einsum('kgl,lkd->kgd', attn_probs, v_row.astype(jnp.float32))
        return attn_vals.reshape(HEADS * HEAD).astype(jnp.bfloat16)

    attn_out = lax.map(one_row, (q_rot, k_all, v_all, seq_lens))
    attn_proj = jnp.dot(attn_out, w_o, preferred_element_type=jnp.float32)
    residual = (tok_hidden.astype(jnp.float32) + attn_proj).astype(jnp.bfloat16)
    mlp_in = rms_norm(residual, g_mlp)
    gate_proj = jnp.dot(mlp_in, w_gate, preferred_element_type=jnp.float32)
    up_proj = jnp.dot(mlp_in, w_up, preferred_element_type=jnp.float32)
    hidden = (jax.nn.silu(gate_proj) * up_proj).astype(jnp.bfloat16)
    down_proj = jnp.dot(hidden, w_down, preferred_element_type=jnp.float32)
    y_out = (residual.astype(jnp.float32) + down_proj).astype(jnp.bfloat16)
    final_norm = rms_norm(y_out, g_final)
    logits = lax.dot_general(final_norm, w_head, (((1,), (1,)), ((), ())), preferred_element_type=jnp.float32)
    norm_lse = jax.nn.logsumexp(logits, axis=-1)
    vocab_ids = jnp.arange(VOCAB)
    target = jnp.sum(jnp.where(vocab_ids[None, :] == next_tok[:, None], logits, 0.0), axis=-1)
    tok_logp = target - norm_lse
    return (y_out, k_all, v_all, tok_logp, norm_lse)
```

```python
import functools
import math

import jax
import jax.numpy as jnp
from jax import lax
from jax.experimental import pallas as pl
from jax.experimental.pallas import tpu as pltpu
from jax.sharding import PartitionSpec as P

THETA = 1000000.0
EPS = 1e-6
BATCH = 256
LMAX = 512
D = 2048
HEAD = 64
FF = 1024
STEP = 16
NSTEP = BATCH // STEP
BLK = STEP * HEAD
NBUF = 8
AHEAD = 5
COL = D // 8
HALF = BATCH // 2
VOC = 16032
VCH = 1024
NFULL = VOC // VCH
VTAIL = VOC - NFULL * VCH
NRING = 9

f32 = jnp.float32
bf16 = jnp.bfloat16
NT = (((1,), (1,)), ((), ()))
MESH = pl.DeviceIdType.MESH


def iota(shape, dim):
    return lax.broadcasted_iota(jnp.int32, shape, dim)


def attn_kernel(len_s, x_hbm, len_hbm, k_hbm, v_hbm, g_hbm, wq_hbm, bq_hbm, wk_hbm, bk_hbm, wv_hbm, bv_hbm, wo_hbm,
                ko_hbm, vo_hbm, part_ref,
                x_v, len_v, g_v, wq_v, bq_v, wkv_v, bk_v, bv_v, wo_v, kbuf, vbuf, normed, knv, qdup, lenc, attn,
                in_sem, krd, vrd, kwr, vwr):
    def load(src, dst, n):
        copy = pltpu.make_async_copy(src, dst, in_sem.at[n])
        copy.start()
        return copy

    small = [
        load(x_hbm, x_v, 0),
        load(g_hbm, g_v, 1),
        load(len_hbm, len_v, 2),
        load(wk_hbm, wkv_v.at[pl.ds(0, HEAD)], 3),
        load(wv_hbm, wkv_v.at[pl.ds(HEAD, HEAD)], 4),
        load(bk_hbm, bk_v, 5),
        load(bv_hbm, bv_v, 6),
        load(wq_hbm, wq_v, 7),
        load(bq_hbm, bq_v, 8),
    ]

    def read(i, hbm, buf, sem):
        slot = lax.rem(i, NBUF)
        return pltpu.make_async_copy(hbm.at[pl.ds(i * BLK, BLK)], buf.at[slot], sem.at[slot])

    def write(i, hbm, buf, sem):
        slot = lax.rem(i, NBUF)
        return pltpu.make_async_copy(buf.at[slot], hbm.at[pl.ds(i * BLK, BLK)], sem.at[slot])

    for i in range(AHEAD):
        read(i, k_hbm, kbuf, krd).start()
        read(i, v_hbm, vbuf, vrd).start()
    wo_copy = load(wo_hbm, wo_v, 9)
    for copy in small:
        copy.wait()

    @pl.loop(0, BATCH // 32)
    def _(r):
        rows = pl.ds(r * 32, 32)
        xr = x_v[rows, :].astype(f32)
        inv = lax.rsqrt(jnp.mean(xr * xr, axis=-1, keepdims=True) + EPS)
        normed[rows, :] = (xr * inv * g_v[...].astype(f32)).astype(bf16)

    freq = jnp.exp(iota((HEAD // 2, BATCH), 0).astype(f32) * (-2.0 / HEAD * math.log(THETA)))
    angles = jnp.broadcast_to(len_v[...].astype(f32), (HEAD // 2, BATCH)) * freq
    cos_t = jnp.cos(angles)
    sin_t = jnp.sin(angles)
    cos_q = jnp.concatenate([cos_t] * 4, axis=0).T
    sin_q = jnp.concatenate([sin_t] * 4, axis=0).T
    lenc[...] = jnp.broadcast_to(len_v[...], (128, BATCH)).astype(f32).T

    bias = jnp.concatenate([bk_v[...].astype(f32), bv_v[...].astype(f32)], axis=1)
    bias = jnp.broadcast_to(bias, (128, 128)).T
    bias = jnp.concatenate([bias, bias], axis=1)
    kv = lax.dot_general(wkv_v[...], normed[...], NT, preferred_element_type=f32) + bias
    first, second = kv[:HEAD // 2], kv[HEAD // 2:HEAD]
    kv = jnp.concatenate([first * cos_t - second * sin_t, second * cos_t + first * sin_t, kv[HEAD:]], axis=0)
    kv = kv.astype(bf16).astype(f32)
    for i in range(NSTEP):
        part = kv[:, (i // 8) * 128:(i // 8) * 128 + 128]
        shift = (128 - STEP * (i % 8)) % 128
        knv[i] = pltpu.roll(part, shift, 1) if shift else part

    q = jnp.dot(normed[...], wq_v[...], preferred_element_type=f32) + bq_v[...].astype(f32)
    lane = iota((BATCH, 128), 1)
    low = lane < HEAD
    early = lax.rem(lane, HEAD) < HEAD // 2
    for j in range(2):
        qa = q[:, j * 128:j * 128 + 128]
        rot = jnp.where(early, -pltpu.roll(qa, 96, 1), pltpu.roll(qa, 32, 1))
        qa = qa * cos_q + rot * sin_q
        swap = pltpu.roll(qa, HEAD, 1)
        qdup[2 * j] = jnp.where(low, qa, swap).astype(bf16)
        qdup[2 * j + 1] = jnp.where(low, swap, qa).astype(bf16)

    @pl.loop(0, NSTEP)
    def _(i):
        slot = lax.rem(i, NBUF)
        nxt = i + AHEAD

        @pl.when(nxt < NSTEP)
        def _():
            @pl.when(nxt >= NBUF)
            def _():
                write(nxt - NBUF, ko_hbm, kbuf, kwr).wait()
                write(nxt - NBUF, vo_hbm, vbuf, vwr).wait()
            read(nxt, k_hbm, kbuf, krd).start()
            read(nxt, v_hbm, vbuf, vrd).start()

        read(i, k_hbm, kbuf, krd).wait()
        read(i, v_hbm, vbuf, vrd).wait()

        lane_l = iota((HEAD, LMAX), 1)
        fresh = knv[i]
        for s in range(STEP):
            here = lane_l == len_s[i * STEP + s]
            rows = pl.ds(s * HEAD, HEAD)
            kcol = jnp.broadcast_to(fresh[:HEAD, s:s + 1], (HEAD, LMAX)).astype(bf16)
            vcol = jnp.broadcast_to(fresh[HEAD:, s:s + 1], (HEAD, LMAX)).astype(bf16)
            kbuf[slot, rows, :] = jnp.where(here, kcol, kbuf[slot, rows, :])
            vbuf[slot, rows, :] = jnp.where(here, vcol, vbuf[slot, rows, :])
        write(i, ko_hbm, kbuf, kwr).start()
        write(i, vo_hbm, vbuf, vwr).start()

        seqs = pl.ds(pl.multiple_of(i * STEP, STEP), STEP)
        diag = iota((STEP, BLK), 1) // HEAD == iota((STEP, BLK), 0)
        lhs = jnp.concatenate(
            [jnp.where(diag, jnp.concatenate([qdup[h, seqs, :]] * 8, axis=1), jnp.zeros((), bf16)) for h in range(4)], axis=0)
        scores = jnp.dot(lhs, kbuf[slot], preferred_element_type=f32) * (HEAD ** -0.5)
        limit = jnp.concatenate([lenc[seqs, :]] * 4, axis=0)
        limit = jnp.concatenate([limit] * 4, axis=1)
        scores = jnp.where(iota((4 * STEP, LMAX), 1).astype(f32) <= limit, scores, -jnp.inf)
        top = jnp.max(scores, axis=-1, keepdims=True)
        expd = jnp.exp(scores - top)
        probs = (expd / jnp.sum(expd, axis=-1, keepdims=True)).astype(bf16)
        out = lax.dot_general(probs, vbuf[slot], NT, preferred_element_type=f32)
        row_s = lax.rem(iota((4 * STEP, 128), 0), STEP)
        lane_s = iota((4 * STEP, 128), 1) // HEAD
        acc = jnp.zeros((4 * STEP, 128), f32)
        for j in range(8):
            acc = acc + jnp.where(row_s == lane_s + 2 * j, out[:, j * 128:j * 128 + 128], 0.0)
        acc = acc + pltpu.roll(acc, HEAD, 1)
        low16 = iota((STEP, 128), 1) < HEAD
        attn[seqs, :] = jnp.concatenate(
            [jnp.where(low16, acc[2 * j * STEP:(2 * j + 1) * STEP], acc[(2 * j + 1) * STEP:(2 * j + 2) * STEP]) for j in range(2)],
            axis=1).astype(bf16)

    wo_copy.wait()
    for d in range(8):
        prod = jnp.dot(attn[...], wo_v[:, d * COL:(d + 1) * COL], preferred_element_type=f32)
        part_ref[d % 2, d // 2] = prod.astype(bf16)
    for i in range(NSTEP - NBUF, NSTEP):
        write(i, ko_hbm, kbuf, kwr).wait()
        write(i, vo_hbm, vbuf, vwr).wait()


def attn_call(lens, x, k, v, g, wq, bq, wk, bk, wv, bv, wo):
    anyspec = pl.BlockSpec(memory_space=pl.ANY)
    cache = jax.ShapeDtypeStruct((BATCH * HEAD, LMAX), bf16)
    return pl.pallas_call(
        attn_kernel,
        out_shape=(cache, cache, jax.ShapeDtypeStruct((2, 4, BATCH, COL), bf16)),
        in_specs=[pl.BlockSpec(memory_space=pltpu.SMEM)] + [anyspec] * 12,
        out_specs=(anyspec, anyspec, pl.BlockSpec(memory_space=pltpu.VMEM)),
        scratch_shapes=[
            pltpu.VMEM((BATCH, D), bf16), pltpu.VMEM((1, BATCH), jnp.int32), pltpu.VMEM((1, D), bf16),
            pltpu.VMEM((D, 4 * HEAD), bf16), pltpu.VMEM((1, 4 * HEAD), bf16), pltpu.VMEM((2 * HEAD, D), bf16),
            pltpu.VMEM((1, HEAD), bf16), pltpu.VMEM((1, HEAD), bf16), pltpu.VMEM((4 * HEAD, D), bf16),
            pltpu.VMEM((NBUF, BLK, LMAX), bf16), pltpu.VMEM((NBUF, BLK, LMAX), bf16),
            pltpu.VMEM((BATCH, D), bf16), pltpu.VMEM((NSTEP, 128, 128), f32), pltpu.VMEM((4, BATCH, 128), bf16),
            pltpu.VMEM((BATCH, 128), f32), pltpu.VMEM((BATCH, 4 * HEAD), bf16),
            pltpu.SemaphoreType.DMA((10,)), pltpu.SemaphoreType.DMA((NBUF,)), pltpu.SemaphoreType.DMA((NBUF,)),
            pltpu.SemaphoreType.DMA((NBUF,)), pltpu.SemaphoreType.DMA((NBUF,)),
        ],
        compiler_params=pltpu.CompilerParams(vmem_limit_bytes=56 * 2**20),
        cost_estimate=pl.CostEstimate(flops=10**10, bytes_accessed=70 * 2**20, transcendentals=10**6),
        name="attn",
    )(lens, x, lens.reshape(1, BATCH), k, v, g, wq, bq, wk, bk, wv, bv, wo)


def tail_kernel(part_ref, x_hbm, tok_ref, gm_ref, gf_ref, wg_hbm, wu_hbm, wd_hbm, wh_hbm,
                y_ref, logp_ref, lse_ref,
                xown, wg_v, wu_v, wd_v, ring, part2, rs1, s2s, s2r, own, afull, yfull, mbuf, hid, fbuf, zbuf, stats, allst,
                in_sem, ring_sem, send_sem, recv_sem, st_send, st_recv):
    me = lax.axis_index("tp")
    core = lax.rem(me, 2)
    chip = me // 2
    partner = me + 1 - 2 * core
    chip_x = chip + 1 - 2 * lax.rem(chip, 2)
    chip_y = chip + 2 - 4 * (chip // 2)
    chip_d = 3 - chip
    others = (chip_x, chip_y, chip_d)

    def load(src, dst, n):
        copy = pltpu.make_async_copy(src, dst, in_sem.at[n])
        copy.start()
        return copy

    cols = pl.ds(pl.multiple_of(me * COL, COL), COL)
    xown_copy = load(x_hbm.at[:, cols], xown, 0)
    wg_copy = load(wg_hbm, wg_v, 1)
    wu_copy = load(wu_hbm, wu_v, 2)
    wd_copy = load(wd_hbm, wd_v, 3)

    def chunk(i):
        slot = lax.rem(i, NRING)
        return pltpu.make_async_copy(wh_hbm.at[pl.ds(i * VCH, VCH)], ring.at[slot], ring_sem.at[slot])

    tail_slot = NFULL % NRING
    tail_copy = pltpu.make_async_copy(wh_hbm.at[pl.ds(NFULL * VCH, VTAIL)], ring.at[tail_slot, pl.ds(0, VTAIL)],
                                      ring_sem.at[tail_slot])
    for i in range(NRING):
        chunk(i).start()

    barrier = pltpu.get_barrier_semaphore()
    for k in range(1, 8):
        pl.semaphore_signal(barrier, inc=1, device_id={"tp": lax.rem(me + k, 8)}, device_id_type=MESH)
    pl.semaphore_wait(barrier, 7)

    def remote(src, dst, n, dev):
        return pltpu.make_async_remote_copy(src_ref=src, dst_ref=dst, send_sem=send_sem.at[n], recv_sem=recv_sem.at[n],
                                            device_id={"tp": dev}, device_id_type=MESH)

    class Reduce:
        def __init__(self, which, half, part, full):
            self.base = (which * 2 + half) * 11
            self.which, self.half, self.part, self.full = which, half, part, full
            self.rows = pl.ds(half * HALF, HALF)

        def s1(self):
            return remote(self.part.at[1 - core, :, self.rows, :], rs1.at[self.which, self.half], self.base, partner)

        def s2(self, k):
            return remote(s2s.at[self.which, self.half, k], s2r.at[self.which, self.half, k], self.base + 1 + k,
                          2 * others[k] + core)

        def s3(self, k):
            block = self.full.at[me, self.rows]
            return remote(block, block, self.base + 4 + k, 2 * others[k] + core)

        def s3own(self):
            block = self.full.at[me, self.rows]
            return remote(block, block, self.base + 7, partner)

        def s4(self, k):
            block = self.full.at[2 * others[k] + core, self.rows]
            return remote(block, block, self.base + 8 + k, partner)

        def scatter(self):
            self.s1().wait_recv()
            for k in (2, 0, 1):
                total = self.part[core, others[k], self.rows, :].astype(f32) + rs1[self.which, self.half, others[k]].astype(f32)
                s2s[self.which, self.half, k] = total.astype(bf16)
                self.s2(k).start()
            own[self.which, self.half] = (self.part[core, chip, self.rows, :].astype(f32)
                                          + rs1[self.which, self.half, chip].astype(f32))

        def gather(self, resid):
            for k in range(3):
                self.s2(k).wait_recv()
            total = resid + own[self.which, self.half]
            for k in range(3):
                total = total + s2r[self.which, self.half, k].astype(f32)
            self.full[me, self.rows, :] = total.astype(bf16)
            for k in (2, 0, 1):
                self.s3(k).start()
            self.s3own().start()

        def forward(self):
            for k in range(3):
                self.s3(k).wait_recv()
                self.s4(k).start()

        def finish(self):
            self.s3own().wait_recv()
            for k in range(3):
                self.s4(k).wait_recv()

        def drain(self):
            self.s1().wait_send()
            self.s3own().wait_send()
            for k in range(3):
                self.s2(k).wait_send()
                self.s3(k).wait_send()
                self.s4(k).wait_send()

    first = [Reduce(0, h, part_ref, afull) for h in range(2)]
    second = [Reduce(1, h, part2, yfull) for h in range(2)]

    def norm_rows(full, half, gain_ref, dst, copy_to=None):
        @pl.loop(0, HALF // 32)
        def _(r):
            rows = pl.ds(pl.multiple_of(half * HALF + r * 32, 32), 32)
            total = jnp.zeros((32, 1), f32)
            for d in range(8):
                block = full[d, rows, :]
                if copy_to is not None:
                    copy_to[rows, d * COL:(d + 1) * COL] = block
                block = block.astype(f32)
                total = total + jnp.sum(block * block, axis=-1, keepdims=True)
            inv = lax.rsqrt(total * (1.0 / D) + EPS)
            for d in range(8):
                gain = gain_ref[:, d * COL:(d + 1) * COL].astype(f32)
                dst[rows, d * COL:(d + 1) * COL] = (full[d, rows, :].astype(f32) * inv * gain).astype(bf16)

    def gate_up(half):
        rows = pl.ds(half * HALF, HALF)
        for n in range(4):
            cs = slice(n * 256, (n + 1) * 256)
            gate = jnp.dot(mbuf[rows, :], wg_v[:, cs], preferred_element_type=f32)
            up = jnp.dot(mbuf[rows, :], wu_v[:, cs], preferred_element_type=f32)
            hid[rows, cs] = (gate / (1.0 + jnp.exp(-gate)) * up).astype(bf16)

    def down(half):
        rows = pl.ds(half * HALF, HALF)
        for d in range(8):
            prod = jnp.dot(hid[rows, :], wd_v[:, d * COL:(d + 1) * COL], preferred_element_type=f32)
            part2[d % 2, d // 2, rows, :] = prod.astype(bf16)

    for h in range(2):
        first[h].s1().start()
    for h in range(2):
        first[h].scatter()
    xown_copy.wait()
    for h in range(2):
        first[h].gather(xown[h * HALF:(h + 1) * HALF, :].astype(f32))
    first[0].forward()
    first[0].finish()
    norm_rows(afull, 0, gm_ref, mbuf)
    wg_copy.wait()
    wu_copy.wait()
    gate_up(0)
    first[1].forward()
    wd_copy.wait()
    down(0)
    second[0].s1().start()
    first[1].finish()
    norm_rows(afull, 1, gm_ref, mbuf)
    second[0].scatter()
    gate_up(1)
    down(1)
    second[1].s1().start()
    second[1].scatter()
    for h in range(2):
        second[h].gather(afull[me, h * HALF:(h + 1) * HALF, :].astype(f32))
    for h in range(2):
        second[h].forward()
    for h in range(2):
        second[h].finish()
        norm_rows(yfull, h, gf_ref, fbuf, y_ref)

    tok = tok_ref[...] - me * VOC

    def score(slot, size, base, state):
        top, total, target = state
        z = lax.dot_general(ring[slot, pl.ds(0, size), :], fbuf[...], NT, preferred_element_type=f32)
        zbuf[pl.ds(0, size), :] = z
        z = zbuf[pl.ds(0, size), :]
        new_top = jnp.maximum(top, jnp.max(z, axis=0, keepdims=True))
        total = total * jnp.exp(top - new_top) + jnp.sum(jnp.exp(z - new_top), axis=0, keepdims=True)
        hit = iota((size, BATCH), 0) == tok - base
        target = target + jnp.sum(jnp.where(hit, z, 0.0), axis=0, keepdims=True)
        return new_top, total, target

    def head_step(i, state):
        chunk(i).wait()
        state = score(lax.rem(i, NRING), VCH, i * VCH, state)
        nxt = i + NRING

        @pl.when(nxt < NFULL)
        def _():
            chunk(nxt).start()

        @pl.when(nxt == NFULL)
        def _():
            tail_copy.start()
        return state

    zero = jnp.zeros((1, BATCH), f32)
    state = (jnp.full((1, BATCH), -jnp.inf, f32), zero, zero)
    state = lax.fori_loop(0, NFULL, head_step, state)
    tail_copy.wait()
    top, total, target = score(tail_slot, VTAIL, NFULL * VCH, state)

    stats[...] = jnp.concatenate([top, total, target, zero, zero, zero, zero, zero], axis=0)
    allst[me] = stats[...]

    def stat_copy(k):
        return pltpu.make_async_remote_copy(src_ref=stats, dst_ref=allst.at[me], send_sem=st_send.at[k - 1],
                                            recv_sem=st_recv.at[k - 1], device_id={"tp": lax.rem(me + k, 8)},
                                            device_id_type=MESH)

    for k in range(1, 8):
        stat_copy(k).start()
    for k in range(1, 8):
        stat_copy(k).wait_recv()
    top = allst[0, 0:1, :]
    for d in range(1, 8):
        top = jnp.maximum(top, allst[d, 0:1, :])
    total = zero
    target = zero
    for d in range(8):
        total = total + allst[d, 1:2, :] * jnp.exp(allst[d, 0:1, :] - top)
        target = target + allst[d, 2:3, :]
    lse = top + jnp.log(total)
    lse_ref[...] = lse
    logp_ref[...] = target - lse
    for h in range(2):
        first[h].drain()
        second[h].drain()
    for k in range(1, 8):
        stat_copy(k).wait_send()


def tail_call(part, x, tok, gm, gf, wg, wu, wd, wh):
    anyspec = pl.BlockSpec(memory_space=pl.ANY)
    vspec = pl.BlockSpec(memory_space=pltpu.VMEM)
    row = jax.ShapeDtypeStruct((1, BATCH), f32)
    blocks = (2, 2, 3, HALF, COL)
    return pl.pallas_call(
        tail_kernel,
        out_shape=(jax.ShapeDtypeStruct((BATCH, D), bf16), row, row),
        in_specs=[vspec, anyspec, vspec, vspec, vspec, anyspec, anyspec, anyspec, anyspec],
        out_specs=(vspec, vspec, vspec),
        scratch_shapes=[
            pltpu.VMEM((BATCH, COL), bf16), pltpu.VMEM((D, FF), bf16), pltpu.VMEM((D, FF), bf16), pltpu.VMEM((FF, D), bf16),
            pltpu.VMEM((NRING, VCH, D), bf16), pltpu.VMEM((2, 4, BATCH, COL), bf16), pltpu.VMEM((2, 2, 4, HALF, COL), bf16),
            pltpu.VMEM(blocks, bf16), pltpu.VMEM(blocks, bf16), pltpu.VMEM((2, 2, HALF, COL), f32),
            pltpu.VMEM((8, BATCH, COL), bf16), pltpu.VMEM((8, BATCH, COL), bf16), pltpu.VMEM((BATCH, D), bf16),
            pltpu.VMEM((BATCH, FF), bf16), pltpu.VMEM((BATCH, D), bf16), pltpu.VMEM((VCH, BATCH), f32),
            pltpu.VMEM((8, BATCH), f32), pltpu.VMEM((8, 8, BATCH), f32),
            pltpu.SemaphoreType.DMA((4,)), pltpu.SemaphoreType.DMA((NRING,)), pltpu.SemaphoreType.DMA((44,)),
            pltpu.SemaphoreType.DMA((44,)), pltpu.SemaphoreType.DMA((7,)), pltpu.SemaphoreType.DMA((7,)),
        ],
        compiler_params=pltpu.CompilerParams(collective_id=0, has_side_effects=True, vmem_limit_bytes=63 * 2**20),
        cost_estimate=pl.CostEstimate(flops=2 * 10**10, bytes_accessed=80 * 2**20, transcendentals=10**6),
        name="tail",
    )(part, x, tok, gm, gf, wg, wu, wd, wh)


def local_step(x, lens, k_cache, v_cache, tok, g_attn, w_q, b_q, w_k, b_k, w_v, b_v, w_o, g_mlp, w_gate, w_up, w_down, g_final, w_head):
    def flat(cache):
        return cache.transpose(0, 2, 3, 1).reshape(BATCH * HEAD, LMAX)

    def unflat(cache):
        return cache.reshape(BATCH, 1, HEAD, LMAX).transpose(0, 3, 1, 2)

    k_new, v_new, part = attn_call(lens, x, flat(k_cache), flat(v_cache), g_attn.reshape(1, D), w_q, b_q.reshape(1, -1),
                                   w_k.T, b_k.reshape(1, -1), w_v.T, b_v.reshape(1, -1), w_o)
    y, logp, lse = tail_call(part, x, tok.reshape(1, BATCH), g_mlp.reshape(1, D), g_final.reshape(1, D), w_gate, w_up, w_down, w_head)
    return y, unflat(k_new), unflat(v_new), logp.reshape(BATCH), lse.reshape(BATCH)


def solution(mesh):
    row_spec = P('dp', None)
    vec_spec = P('dp')
    cache_spec = P('dp', None, 'tp', None)
    col_spec = P(None, 'tp')
    part_spec = P('tp')
    whole_spec = P(None)
    in_specs = (row_spec, vec_spec, cache_spec, cache_spec, vec_spec, whole_spec, col_spec, part_spec, col_spec, part_spec, col_spec, part_spec, P('tp', None), whole_spec, col_spec, col_spec, P('tp', None), whole_spec, P('tp', None))
    out_specs = (row_spec, cache_spec, cache_spec, vec_spec, vec_spec)
    return jax.shard_map(local_step, mesh=mesh, in_specs=in_specs, out_specs=out_specs, check_vma=False)
```

```python
import functools
import math

import jax
import jax.numpy as jnp
from jax import lax
from jax.experimental import pallas as pl
from jax.experimental.pallas import tpu as pltpu
from jax.sharding import PartitionSpec as P

THETA = 1000000.0
EPS = 1e-6
BATCH = 256
LMAX = 512
D = 2048
HEAD = 64
FF = 1024
STEP = 16
NSTEP = BATCH // STEP
BLK = STEP * HEAD
NPAIR = NSTEP // 2
HOLD = 2
COL = D // 8
HALF = BATCH // 2
VOC = 16032
VCH = 1024
NFULL = VOC // VCH
VTAIL = VOC - NFULL * VCH
NRING = 7
SUB = 256
GROUP = 3

f32 = jnp.float32
bf16 = jnp.bfloat16
NT = (((1,), (1,)), ((), ()))
MESH = pl.DeviceIdType.MESH


def iota(shape, dim):
    return lax.broadcasted_iota(jnp.int32, shape, dim)


def row_of(ref, start, count):
    return jnp.concatenate([ref[start + i:start + i + 1, :] for i in range(count)], axis=1).astype(f32)


def inverse_rms(pieces):
    squares = [piece * piece for piece in pieces]
    while len(squares) > 1:
        squares = [squares[i] + squares[i + 1] for i in range(0, len(squares), 2)]
    return lax.rsqrt(jnp.sum(squares[0], axis=-1, keepdims=True) * (1.0 / D) + EPS)


def attn_kernel(len_s, x_hbm, len_hbm, k_hbm, v_hbm, g_hbm, wq_hbm, bq_hbm, wk_hbm, bk_hbm, wv_hbm, bv_hbm, wo_hbm,
                ko_hbm, vo_hbm, part_ref,
                x_v, len_v, g_v, wq_v, bq_v, wkv_v, bk_v, bv_v, wo_v, kbuf0, kbuf1, vbuf0, vbuf1, normed, knv, qdup, lenc, attn,
                in_sem, rd_sem, wr_sem):
    def load(src, dst, n):
        copy = pltpu.make_async_copy(src, dst, in_sem.at[n])
        copy.start()
        return copy

    scope = jax.named_scope
    small = [
        load(x_hbm, x_v, 0),
        load(g_hbm, g_v, 1),
        load(len_hbm, len_v, 2),
        load(wk_hbm, wkv_v.at[pl.ds(0, HEAD)], 3),
        load(wv_hbm, wkv_v.at[pl.ds(HEAD, HEAD)], 4),
        load(bk_hbm, bk_v, 5),
        load(bv_hbm, bv_v, 6),
        load(wq_hbm, wq_v, 7),
        load(bq_hbm, bq_v, 8),
    ]

    kbuf, vbuf = (kbuf0, kbuf1), (vbuf0, vbuf1)

    def reads(p, j):
        rows = pl.ds((2 * j + p) * BLK, BLK)
        return (pltpu.make_async_copy(k_hbm.at[rows], kbuf[p].at[j], rd_sem.at[p, j]),
                pltpu.make_async_copy(v_hbm.at[rows], vbuf[p].at[j], rd_sem.at[2 + p, j]))

    def writes(p, j):
        rows = pl.ds((2 * j + p) * BLK, BLK)
        return (pltpu.make_async_copy(kbuf[p].at[j], ko_hbm.at[rows], wr_sem.at[p, j]),
                pltpu.make_async_copy(vbuf[p].at[j], vo_hbm.at[rows], wr_sem.at[2 + p, j]))

    def start(copies):
        for copy in copies:
            copy.start()

    def wait(copies):
        for copy in copies:
            copy.wait()

    start(reads(0, 0))
    start(reads(1, 0))
    with scope("loads"):
        for copy in small:
            copy.wait()
    for j in range(1, NPAIR):
        start(reads(0, j))
        start(reads(1, j))
    wo_copy = load(wo_hbm, wo_v, 9)

    @pl.loop(0, BATCH // 32)
    @scope("norm")
    def _(r):
        rows = pl.ds(pl.multiple_of(r * 32, 32), 32)
        xs = [x_v[rows, d * 128:(d + 1) * 128].astype(f32) for d in range(16)]
        inv = inverse_rms(xs)
        for d in range(16):
            normed[rows, d * 128:(d + 1) * 128] = (xs[d] * inv * row_of(g_v, d, 1)).astype(bf16)

    freq = jnp.exp(iota((HEAD // 2, BATCH), 0).astype(f32) * (-2.0 / HEAD * math.log(THETA)))
    angles = jnp.broadcast_to(len_v[...].astype(f32), (HEAD // 2, BATCH)) * freq
    cos_t = jnp.cos(angles)
    sin_t = jnp.sin(angles)
    cos_q = jnp.concatenate([cos_t] * 4, axis=0).T
    sin_q = jnp.concatenate([sin_t] * 4, axis=0).T
    lenc[...] = jnp.broadcast_to(len_v[...], (128, BATCH)).astype(f32).T

    bias = jnp.concatenate([bk_v[...].astype(f32), bv_v[...].astype(f32)], axis=1)
    bias = jnp.broadcast_to(bias, (128, 128)).T
    bias = jnp.concatenate([bias, bias], axis=1)
    kv = lax.dot_general(wkv_v[...], normed[...], NT, preferred_element_type=f32) + bias
    first, second = kv[:HEAD // 2], kv[HEAD // 2:HEAD]
    kv = jnp.concatenate([first * cos_t - second * sin_t, second * cos_t + first * sin_t, kv[HEAD:]], axis=0)
    kv = kv.astype(bf16).astype(f32)
    for i in range(NSTEP):
        part = kv[:, (i // 8) * 128:(i // 8) * 128 + 128]
        shift = (128 - STEP * (i % 8)) % 128
        knv[i] = pltpu.roll(part, shift, 1) if shift else part

    q = jnp.dot(normed[...], wq_v[...], preferred_element_type=f32) + row_of(bq_v, 0, 2)
    lane = iota((BATCH, 128), 1)
    low = lane < HEAD
    early = lax.rem(lane, HEAD) < HEAD // 2
    for j in range(2):
        qa = q[:, j * 128:j * 128 + 128]
        rot = jnp.where(early, -pltpu.roll(qa, 96, 1), pltpu.roll(qa, 32, 1))
        qa = qa * cos_q + rot * sin_q
        swap = pltpu.roll(qa, HEAD, 1)
        qdup[2 * j] = jnp.where(low, qa, swap).astype(bf16)
        qdup[2 * j + 1] = jnp.where(low, swap, qa).astype(bf16)

    def update(p, j):
        i = 2 * j + p
        lane_l = iota((HEAD, LMAX), 1)
        fresh = knv[i]
        for s in range(STEP):
            here = lane_l == len_s[i * STEP + s]
            rows = pl.ds(s * HEAD, HEAD)
            kcol = jnp.broadcast_to(fresh[:HEAD, s:s + 1], (HEAD, LMAX)).astype(bf16)
            vcol = jnp.broadcast_to(fresh[HEAD:, s:s + 1], (HEAD, LMAX)).astype(bf16)
            kbuf[p][j, rows, :] = jnp.where(here, kcol, kbuf[p][j, rows, :])
            vbuf[p][j, rows, :] = jnp.where(here, vcol, vbuf[p][j, rows, :])

    def attend(p, j):
        seqs = pl.ds(pl.multiple_of((2 * j + p) * STEP, STEP), STEP)
        diag = iota((STEP, BLK), 1) // HEAD == iota((STEP, BLK), 0)
        lhs = jnp.concatenate(
            [jnp.where(diag, jnp.concatenate([qdup[h, seqs, :]] * 8, axis=1), jnp.zeros((), bf16)) for h in range(4)], axis=0)
        scores = jnp.dot(lhs, kbuf[p][j], preferred_element_type=f32) * (HEAD ** -0.5)
        limit = jnp.concatenate([lenc[seqs, :]] * 4, axis=0)
        limit = jnp.concatenate([limit] * 4, axis=1)
        scores = jnp.where(iota((4 * STEP, LMAX), 1).astype(f32) <= limit, scores, -jnp.inf)
        top = jnp.max(scores, axis=-1, keepdims=True)
        expd = jnp.exp(scores - top)
        probs = (expd / jnp.sum(expd, axis=-1, keepdims=True)).astype(bf16)
        out = lax.dot_general(probs, vbuf[p][j], NT, preferred_element_type=f32)
        row_s = lax.rem(iota((4 * STEP, 128), 0), STEP)
        lane_s = iota((4 * STEP, 128), 1) // HEAD
        acc = jnp.zeros((4 * STEP, 128), f32)
        for t in range(8):
            acc = acc + jnp.where(row_s == lane_s + 2 * t, out[:, t * 128:t * 128 + 128], 0.0)
        acc = acc + pltpu.roll(acc, HEAD, 1)
        low16 = iota((STEP, 128), 1) < HEAD
        attn[seqs, :] = jnp.concatenate(
            [jnp.where(low16, acc[2 * t * STEP:(2 * t + 1) * STEP], acc[(2 * t + 1) * STEP:(2 * t + 2) * STEP]) for t in range(2)],
            axis=1).astype(bf16)

    wait(reads(0, 0))
    with scope("update"):
        update(0, 0)

    @pl.loop(0, NPAIR - 1)
    def _(j):
        with scope("kvwait"):
            wait(reads(1, j))
        with scope("pair"):
            update(1, j)
            attend(0, j)
        with scope("kvwait"):
            wait(reads(0, j + 1))
        with scope("pair"):
            update(0, j + 1)
            attend(1, j)

        @pl.when(j == HOLD)
        def _():
            for jj in range(HOLD + 1):
                start(writes(0, jj))
                start(writes(1, jj))

        @pl.when(j > HOLD)
        def _():
            start(writes(0, j))
            start(writes(1, j))

    wait(reads(1, NPAIR - 1))
    with scope("pair"):
        update(1, NPAIR - 1)
        start(writes(0, NPAIR - 1))
        start(writes(1, NPAIR - 1))
        attend(0, NPAIR - 1)
        attend(1, NPAIR - 1)

    wo_copy.wait()
    for d in range(8):
        prod = jnp.dot(attn[...], wo_v[:, d * COL:(d + 1) * COL], preferred_element_type=f32)
        part_ref[d % 2, d // 2] = prod.astype(bf16)
    with scope("drain"):
        for j in range(NPAIR):
            wait(writes(0, j))
            wait(writes(1, j))


def attn_call(lens, x, k, v, g, wq, bq, wk, bk, wv, bv, wo):
    anyspec = pl.BlockSpec(memory_space=pl.ANY)
    cache = jax.ShapeDtypeStruct((BATCH * HEAD, LMAX), bf16)
    return pl.pallas_call(
        attn_kernel,
        out_shape=(cache, cache, pltpu.VMEM((2, 4, BATCH, COL), bf16)),
        in_specs=[pl.BlockSpec(memory_space=pltpu.SMEM)] + [anyspec] * 12,
        out_specs=(anyspec, anyspec, pl.BlockSpec(memory_space=pltpu.VMEM)),
        scratch_shapes=[
            pltpu.VMEM((BATCH, D), bf16), pltpu.VMEM((1, BATCH), jnp.int32), pltpu.VMEM((16, 128), bf16),
            pltpu.VMEM((D, 4 * HEAD), bf16), pltpu.VMEM((2, 128), bf16), pltpu.VMEM((2 * HEAD, D), bf16),
            pltpu.VMEM((1, HEAD), bf16), pltpu.VMEM((1, HEAD), bf16), pltpu.VMEM((4 * HEAD, D), bf16),
            *[pltpu.VMEM((NPAIR, BLK, LMAX), bf16)] * 4,
            pltpu.VMEM((BATCH, D), bf16), pltpu.VMEM((NSTEP, 128, 128), f32), pltpu.VMEM((4, BATCH, 128), bf16),
            pltpu.VMEM((BATCH, 128), f32), pltpu.VMEM((BATCH, 4 * HEAD), bf16),
            pltpu.SemaphoreType.DMA((10,)), pltpu.SemaphoreType.DMA((4, NPAIR)), pltpu.SemaphoreType.DMA((4, NPAIR)),
        ],
        compiler_params=pltpu.CompilerParams(vmem_limit_bytes=56 * 2**20),
        cost_estimate=pl.CostEstimate(flops=10**10, bytes_accessed=70 * 2**20, transcendentals=10**6),
        name="attn",
    )(lens, x, lens.reshape(1, BATCH), k, v, g, wq, bq, wk, bk, wv, bv, wo)


def meet(me):
    barrier = pltpu.get_barrier_semaphore()
    for k in range(1, 8):
        pl.semaphore_signal(barrier, inc=1, device_id={"tp": lax.rem(me + k, 8)}, device_id_type=MESH)
    pl.semaphore_wait(barrier, 7)


def tail_kernel(part_ref, x_hbm, tok_ref, gm_ref, gf_ref, wg_hbm, wu_hbm, wd_hbm, wh_hbm,
                y_ref, out_ref,
                xown, wg_v, wu_v, wd_v, ring, part2, rs1, s2s, s2r, own, afull, yfull, mbuf, hid, fbuf, fturn, zbuf, stats, allst,
                in_sem, ring_sem, send_sem, recv_sem, st_send, st_recv):
    me = lax.axis_index("tp")
    core = lax.rem(me, 2)
    chip = me // 2
    partner = me + 1 - 2 * core
    chip_x = chip + 1 - 2 * lax.rem(chip, 2)
    chip_y = chip + 2 - 4 * (chip // 2)
    chip_d = 3 - chip
    others = (chip_x, chip_y, chip_d)

    def load(src, dst, n):
        copy = pltpu.make_async_copy(src, dst, in_sem.at[n])
        copy.start()
        return copy

    cols = pl.ds(pl.multiple_of(me * COL, COL), COL)
    xown_copy = load(x_hbm.at[:, cols], xown, 0)
    wg_copy = load(wg_hbm, wg_v, 1)
    wu_copy = load(wu_hbm, wu_v, 2)
    wd_copy = load(wd_hbm, wd_v, 3)

    def chunk(i):
        slot = lax.rem(i, NRING)
        return pltpu.make_async_copy(wh_hbm.at[pl.ds(i * VCH, VCH)], ring.at[slot], ring_sem.at[slot])

    tail_slot = NFULL % NRING
    tail_copy = pltpu.make_async_copy(wh_hbm.at[pl.ds(NFULL * VCH, VTAIL)], ring.at[tail_slot, pl.ds(0, VTAIL)],
                                      ring_sem.at[tail_slot])
    for i in range(NRING):
        chunk(i).start()

    with jax.named_scope('barrier'):
        meet(me)

    def remote(src, dst, n, dev):
        return pltpu.make_async_remote_copy(src_ref=src, dst_ref=dst, send_sem=send_sem.at[n], recv_sem=recv_sem.at[n],
                                            device_id={"tp": dev}, device_id_type=MESH)

    class Reduce:
        def __init__(self, which, half, part, full):
            self.base = (which * 2 + half) * 11
            self.which, self.half, self.part, self.full = which, half, part, full
            self.rows = pl.ds(half * HALF, HALF)

        def s1(self):
            return remote(self.part.at[1 - core, :, self.rows, :], rs1.at[self.which, self.half], self.base, partner)

        def s2(self, k):
            return remote(s2s.at[self.which, self.half, k], s2r.at[self.which, self.half, k], self.base + 1 + k,
                          2 * others[k] + core)

        def s3(self, k):
            block = self.full.at[me, self.rows]
            return remote(block, block, self.base + 4 + k, 2 * others[k] + core)

        def s3own(self):
            block = self.full.at[me, self.rows]
            return remote(block, block, self.base + 7, partner)

        def s4(self, k):
            block = self.full.at[2 * others[k] + core, self.rows]
            return remote(block, block, self.base + 8 + k, partner)

        @jax.named_scope('scatter')
        def scatter(self):
            self.s1().wait_recv()
            for k in (2, 0, 1):
                total = self.part[core, others[k], self.rows, :].astype(f32) + rs1[self.which, self.half, others[k]].astype(f32)
                s2s[self.which, self.half, k] = total.astype(bf16)
                self.s2(k).start()
            own[self.which, self.half] = (self.part[core, chip, self.rows, :].astype(f32)
                                          + rs1[self.which, self.half, chip].astype(f32))

        @jax.named_scope('gather')
        def gather(self, resid):
            for k in range(3):
                self.s2(k).wait_recv()
            total = resid + own[self.which, self.half]
            for k in range(3):
                total = total + s2r[self.which, self.half, k].astype(f32)
            self.full[me, self.rows, :] = total.astype(bf16)
            for k in (2, 0, 1):
                self.s3(k).start()
            self.s3own().start()

        @jax.named_scope('forward')
        def forward(self):
            for k in range(3):
                self.s3(k).wait_recv()
                self.s4(k).start()

        @jax.named_scope('finish')
        def finish(self):
            self.s3own().wait_recv()
            for k in range(3):
                self.s4(k).wait_recv()

        def drain(self):
            self.s1().wait_send()
            self.s3own().wait_send()
            for k in range(3):
                self.s2(k).wait_send()
                self.s3(k).wait_send()
                self.s4(k).wait_send()

    first = [Reduce(0, h, part_ref, afull) for h in range(2)]
    second = [Reduce(1, h, part2, yfull) for h in range(2)]

    @jax.named_scope('norm_rows')
    def norm_rows(full, half, gain_ref, dst, copy_to=None):
        @pl.loop(0, HALF // 32)
        def _(r):
            rows = pl.ds(pl.multiple_of(half * HALF + r * 32, 32), 32)
            xs = []
            for d in range(16):
                block = full[d // 2, rows, (d % 2) * 128:(d % 2) * 128 + 128]
                if copy_to is not None:
                    copy_to[rows, d * 128:(d + 1) * 128] = block
                xs.append(block.astype(f32))
            inv = inverse_rms(xs)
            for d in range(16):
                dst[rows, d * 128:(d + 1) * 128] = (xs[d] * inv * row_of(gain_ref, d, 1)).astype(bf16)

    @jax.named_scope('gate_up')
    def gate_up(half, between=None):
        rows = pl.ds(half * HALF, HALF)
        for n in range(4):
            if n == 3 and between is not None:
                between()
            cs = slice(n * 256, (n + 1) * 256)
            gate = jnp.dot(mbuf[rows, :], wg_v[:, cs], preferred_element_type=f32)
            up = jnp.dot(mbuf[rows, :], wu_v[:, cs], preferred_element_type=f32)
            hid[rows, cs] = (gate / (1.0 + jnp.exp(-gate)) * up).astype(bf16)

    @jax.named_scope('down')
    def down(half):
        rows = pl.ds(half * HALF, HALF)
        for d in range(8):
            prod = jnp.dot(hid[rows, :], wd_v[:, d * COL:(d + 1) * COL], preferred_element_type=f32)
            part2[d % 2, d // 2, rows, :] = prod.astype(bf16)

    for h in range(2):
        first[h].s1().start()
    for h in range(2):
        first[h].scatter()
    xown_copy.wait()
    for h in range(2):
        first[h].gather(xown[h * HALF:(h + 1) * HALF, :].astype(f32))
    first[0].forward()
    first[0].finish()
    norm_rows(afull, 0, gm_ref, mbuf)
    wg_copy.wait()
    wu_copy.wait()
    gate_up(0, first[1].forward)
    wd_copy.wait()
    down(0)
    second[0].s1().start()
    first[1].finish()
    norm_rows(afull, 1, gm_ref, mbuf)
    second[0].scatter()
    gate_up(1)
    down(1)
    second[1].s1().start()
    second[1].scatter()
    for h in range(2):
        second[h].gather(afull[me, h * HALF:(h + 1) * HALF, :].astype(f32))
    for h in range(2):
        second[h].forward()
        second[h].finish()
        norm_rows(yfull, h, gf_ref, fbuf, y_ref)
        with jax.named_scope("turn"):
            for d in range(8):
                cs = slice(d * COL, (d + 1) * COL)
                fturn[cs, h * HALF:(h + 1) * HALF] = fbuf[h * HALF:(h + 1) * HALF, cs].T

    tok = jnp.broadcast_to(tok_ref[...] - me * VOC, (8, BATCH))

    def absorb(buf, size, base, state):
        top, total, target = state
        z = zbuf[buf, pl.ds(0, size), :].reshape(size // 8, 8, BATCH)
        new_top = jnp.maximum(top, jnp.max(z, axis=0))
        total = total * jnp.exp(top - new_top) + jnp.sum(jnp.exp(z - new_top[None]), axis=0)
        hit = iota(z.shape, 0) * 8 + iota(z.shape, 1) == (tok - base)[None]
        target = target + jnp.sum(jnp.where(hit, z, 0.0), axis=0)
        return new_top, total, target

    def score(slot, size, base, state, before):
        for n, start in enumerate(range(0, size, SUB)):
            rows = min(SUB, size - start)
            z = jnp.dot(ring[slot, pl.ds(start, rows), :], fturn[...], preferred_element_type=f32)
            state = absorb((n + 1) % 2, SUB, before if n == 0 else base + start - SUB, state)
            zbuf[n % 2, pl.ds(0, rows), :] = z
        return state

    def head_step(t, state):
        with jax.named_scope('hwait'):
            for u in range(GROUP):
                chunk(t * GROUP + u).wait()
        for u in range(GROUP):
            i = t * GROUP + u
            before = jnp.where(i == 0, -2 * BATCH * VOC, i * VCH - SUB)
            state = score(lax.rem(i, NRING), VCH, i * VCH, state, before)
        for u in range(GROUP):
            nxt = t * GROUP + u + NRING

            @pl.when(nxt < NFULL)
            def _():
                chunk(nxt).start()

            @pl.when(nxt == NFULL)
            def _():
                tail_copy.start()
        return state

    zero = jnp.zeros((8, BATCH), f32)
    zbuf[1] = jnp.full((SUB, BATCH), -jnp.inf, f32)
    state = (jnp.full((8, BATCH), jnp.finfo(jnp.float32).min, f32), zero, zero)
    state = lax.fori_loop(0, NFULL // GROUP, head_step, state)
    tail_copy.wait()
    state = score(tail_slot, VTAIL, NFULL * VCH, state, NFULL * VCH - SUB)
    last = (VTAIL - 1) // SUB
    top8, total8, target8 = absorb(last % 2, VTAIL - last * SUB, NFULL * VCH + last * SUB, state)
    top = jnp.max(top8, axis=0, keepdims=True)
    total = jnp.sum(total8 * jnp.exp(top8 - top), axis=0, keepdims=True)
    target = jnp.sum(target8, axis=0, keepdims=True)
    zero = jnp.zeros((1, BATCH), f32)

    stats[...] = jnp.concatenate([top, total, target, zero, zero, zero, zero, zero], axis=0)
    allst[me] = stats[...]

    def stat_copy(k):
        return pltpu.make_async_remote_copy(src_ref=stats, dst_ref=allst.at[me], send_sem=st_send.at[k - 1],
                                            recv_sem=st_recv.at[k - 1], device_id={"tp": lax.rem(me + k, 8)},
                                            device_id_type=MESH)

    for k in range(1, 8):
        stat_copy(k).start()
    with jax.named_scope('statwait'):
        for k in range(1, 8):
            stat_copy(k).wait_recv()
    out_ref[...] = allst[...]
    for h in range(2):
        first[h].drain()
        second[h].drain()
    for k in range(1, 8):
        stat_copy(k).wait_send()


def tail_call(part, x, tok, gm, gf, wg, wu, wd, wh):
    anyspec = pl.BlockSpec(memory_space=pl.ANY)
    vspec = pl.BlockSpec(memory_space=pltpu.VMEM)
    blocks = (2, 2, 3, HALF, COL)
    return pl.pallas_call(
        tail_kernel,
        out_shape=(pltpu.VMEM((BATCH, D), bf16), pltpu.VMEM((8, 8, BATCH), f32)),
        in_specs=[vspec, anyspec, vspec, vspec, vspec, anyspec, anyspec, anyspec, anyspec],
        out_specs=(vspec, vspec),
        scratch_shapes=[
            pltpu.VMEM((BATCH, COL), bf16), pltpu.VMEM((D, FF), bf16), pltpu.VMEM((D, FF), bf16), pltpu.VMEM((FF, D), bf16),
            pltpu.VMEM((NRING, VCH, D), bf16), pltpu.VMEM((2, 4, BATCH, COL), bf16), pltpu.VMEM((2, 2, 4, HALF, COL), bf16),
            pltpu.VMEM(blocks, bf16), pltpu.VMEM(blocks, bf16), pltpu.VMEM((2, 2, HALF, COL), f32),
            pltpu.VMEM((8, BATCH, COL), bf16), pltpu.VMEM((8, BATCH, COL), bf16), pltpu.VMEM((BATCH, D), bf16),
            pltpu.VMEM((BATCH, FF), bf16), pltpu.VMEM((BATCH, D), bf16), pltpu.VMEM((D, BATCH), bf16), pltpu.VMEM((2, SUB, BATCH), f32),
            pltpu.VMEM((8, BATCH), f32), pltpu.VMEM((8, 8, BATCH), f32),
            pltpu.SemaphoreType.DMA((4,)), pltpu.SemaphoreType.DMA((NRING,)), pltpu.SemaphoreType.DMA((44,)),
            pltpu.SemaphoreType.DMA((44,)), pltpu.SemaphoreType.DMA((7,)), pltpu.SemaphoreType.DMA((7,)),
        ],
        compiler_params=pltpu.CompilerParams(collective_id=0, has_side_effects=True, vmem_limit_bytes=54 * 2**20),
        cost_estimate=pl.CostEstimate(flops=2 * 10**10, bytes_accessed=80 * 2**20, transcendentals=10**6),
        name="tail",
    )(pltpu.with_memory_space_constraint(part, pltpu.VMEM), x, tok, gm, gf, wg, wu, wd, wh)


def end_kernel(y_ref, allst, y_hbm, logp_ref, lse_ref, sem):
    copy = pltpu.make_async_copy(y_ref, y_hbm, sem)
    copy.start()
    top = allst[0, 0:1, :]
    for d in range(1, 8):
        top = jnp.maximum(top, allst[d, 0:1, :])
    total = jnp.zeros((1, BATCH), f32)
    target = jnp.zeros((1, BATCH), f32)
    for d in range(8):
        total = total + allst[d, 1:2, :] * jnp.exp(allst[d, 0:1, :] - top)
        target = target + allst[d, 2:3, :]
    lse = top + jnp.log(total)
    lse_ref[...] = lse
    logp_ref[...] = target - lse
    copy.wait()


def end_call(y, stats):
    vspec = pl.BlockSpec(memory_space=pltpu.VMEM)
    row = jax.ShapeDtypeStruct((1, BATCH), f32)
    return pl.pallas_call(
        end_kernel,
        out_shape=(jax.ShapeDtypeStruct((BATCH, D), bf16), row, row),
        in_specs=[vspec, vspec],
        out_specs=(pl.BlockSpec(memory_space=pl.ANY), vspec, vspec),
        scratch_shapes=[pltpu.SemaphoreType.DMA],
        compiler_params=pltpu.CompilerParams(vmem_limit_bytes=4 * 2**20),
        name="end",
    )(y, stats)


def local_step(x, lens, k_cache, v_cache, tok, g_attn, w_q, b_q, w_k, b_k, w_v, b_v, w_o, g_mlp, w_gate, w_up, w_down, g_final, w_head):
    def flat(cache):
        return cache.transpose(0, 2, 3, 1).reshape(BATCH * HEAD, LMAX)

    def unflat(cache):
        return cache.reshape(BATCH, 1, HEAD, LMAX).transpose(0, 3, 1, 2)

    k_new, v_new, part = attn_call(lens, x, flat(k_cache), flat(v_cache), g_attn.reshape(16, 128), w_q, b_q.reshape(2, 128),
                                   w_k.T, b_k.reshape(1, -1), w_v.T, b_v.reshape(1, -1), w_o)
    y, logp, lse = end_call(*tail_call(part, x, tok.reshape(1, BATCH), g_mlp.reshape(16, 128), g_final.reshape(16, 128), w_gate, w_up, w_down, w_head))
    return y, unflat(k_new), unflat(v_new), logp.reshape(BATCH), lse.reshape(BATCH)


def solution(mesh):
    row_spec = P('dp', None)
    vec_spec = P('dp')
    cache_spec = P('dp', None, 'tp', None)
    col_spec = P(None, 'tp')
    part_spec = P('tp')
    whole_spec = P(None)
    in_specs = (row_spec, vec_spec, cache_spec, cache_spec, vec_spec, whole_spec, col_spec, part_spec, col_spec, part_spec, col_spec, part_spec, P('tp', None), whole_spec, col_spec, col_spec, P('tp', None), whole_spec, P('tp', None))
    out_specs = (row_spec, cache_spec, cache_spec, vec_spec, vec_spec)
    return jax.shard_map(local_step, mesh=mesh, in_specs=in_specs, out_specs=out_specs, check_vma=False)
```

```python
import functools
import math

import jax
import jax.numpy as jnp
from jax import lax
from jax.experimental import pallas as pl
from jax.experimental.pallas import tpu as pltpu
from jax.sharding import PartitionSpec as P

THETA = 1000000.0
EPS = 1e-6
BATCH = 256
LMAX = 512
D = 2048
HEAD = 64
FF = 1024
STEP = 16
NSTEP = BATCH // STEP
BLK = STEP * HEAD
NPAIR = NSTEP // 2
HOLD = 2
COL = D // 8
HALF = BATCH // 2
NMSG = 11
AT = 1
VOC = 16032
VCH = 1024
NFULL = VOC // VCH
VTAIL = VOC - NFULL * VCH
NRING = 7
SUB = 256
GROUP = 3

f32 = jnp.float32
bf16 = jnp.bfloat16
NT = (((1,), (1,)), ((), ()))
MESH = pl.DeviceIdType.MESH


def iota(shape, dim):
    return lax.broadcasted_iota(jnp.int32, shape, dim)


def row_of(ref, start, count):
    return jnp.concatenate([ref[start + i:start + i + 1, :] for i in range(count)], axis=1).astype(f32)


def inverse_rms(pieces):
    squares = [piece * piece for piece in pieces]
    while len(squares) > 1:
        squares = [squares[i] + squares[i + 1] for i in range(0, len(squares), 2)]
    return lax.rsqrt(jnp.sum(squares[0], axis=-1, keepdims=True) * (1.0 / D) + EPS)


def attn_kernel(len_s, x_hbm, len_hbm, k_hbm, v_hbm, g_hbm, wq_hbm, bq_hbm, wk_hbm, bk_hbm, wv_hbm, bv_hbm, wo_hbm,
                ko_hbm, vo_hbm, part_ref,
                x_v, len_v, g_v, wq_v, bq_v, wkv_v, bk_v, bv_v, wo_v, kbuf0, kbuf1, vbuf0, vbuf1, normed, knv, qdup, lenc, attn,
                in_sem, rd_sem, wr_sem):
    def load(src, dst, n):
        copy = pltpu.make_async_copy(src, dst, in_sem.at[n])
        copy.start()
        return copy

    scope = jax.named_scope
    small = [
        load(x_hbm, x_v, 0),
        load(g_hbm, g_v, 1),
        load(len_hbm, len_v, 2),
        load(wk_hbm, wkv_v.at[pl.ds(0, HEAD)], 3),
        load(wv_hbm, wkv_v.at[pl.ds(HEAD, HEAD)], 4),
        load(bk_hbm, bk_v, 5),
        load(bv_hbm, bv_v, 6),
        load(wq_hbm, wq_v, 7),
        load(bq_hbm, bq_v, 8),
    ]

    kbuf, vbuf = (kbuf0, kbuf1), (vbuf0, vbuf1)

    def reads(p, j):
        rows = pl.ds((2 * j + p) * BLK, BLK)
        return (pltpu.make_async_copy(k_hbm.at[rows], kbuf[p].at[j], rd_sem.at[p, j]),
                pltpu.make_async_copy(v_hbm.at[rows], vbuf[p].at[j], rd_sem.at[2 + p, j]))

    def writes(p, j):
        rows = pl.ds((2 * j + p) * BLK, BLK)
        return (pltpu.make_async_copy(kbuf[p].at[j], ko_hbm.at[rows], wr_sem.at[p, j]),
                pltpu.make_async_copy(vbuf[p].at[j], vo_hbm.at[rows], wr_sem.at[2 + p, j]))

    def start(copies):
        for copy in copies:
            copy.start()

    def wait(copies):
        for copy in copies:
            copy.wait()

    start(reads(0, 0))
    start(reads(1, 0))
    with scope("loads"):
        for copy in small:
            copy.wait()
    for j in range(1, NPAIR):
        start(reads(0, j))
        start(reads(1, j))
    wo_copy = load(wo_hbm, wo_v, 9)

    @pl.loop(0, BATCH // 32)
    @scope("norm")
    def _(r):
        rows = pl.ds(pl.multiple_of(r * 32, 32), 32)
        xs = [x_v[rows, d * 128:(d + 1) * 128].astype(f32) for d in range(16)]
        inv = inverse_rms(xs)
        for d in range(16):
            normed[rows, d * 128:(d + 1) * 128] = (xs[d] * inv * row_of(g_v, d, 1)).astype(bf16)

    freq = jnp.exp(iota((HEAD // 2, BATCH), 0).astype(f32) * (-2.0 / HEAD * math.log(THETA)))
    angles = jnp.broadcast_to(len_v[...].astype(f32), (HEAD // 2, BATCH)) * freq
    cos_t = jnp.cos(angles)
    sin_t = jnp.sin(angles)
    cos_q = jnp.concatenate([cos_t] * 4, axis=0).T
    sin_q = jnp.concatenate([sin_t] * 4, axis=0).T
    lenc[...] = jnp.broadcast_to(len_v[...], (128, BATCH)).astype(f32).T

    bias = jnp.concatenate([bk_v[...].astype(f32), bv_v[...].astype(f32)], axis=1)
    bias = jnp.broadcast_to(bias, (128, 128)).T
    bias = jnp.concatenate([bias, bias], axis=1)
    kv = lax.dot_general(wkv_v[...], normed[...], NT, preferred_element_type=f32) + bias
    first, second = kv[:HEAD // 2], kv[HEAD // 2:HEAD]
    kv = jnp.concatenate([first * cos_t - second * sin_t, second * cos_t + first * sin_t, kv[HEAD:]], axis=0)
    kv = kv.astype(bf16).astype(f32)
    for i in range(NSTEP):
        part = kv[:, (i // 8) * 128:(i // 8) * 128 + 128]
        shift = (128 - STEP * (i % 8)) % 128
        knv[i] = pltpu.roll(part, shift, 1) if shift else part

    q = jnp.dot(normed[...], wq_v[...], preferred_element_type=f32) + row_of(bq_v, 0, 2)
    lane = iota((BATCH, 128), 1)
    low = lane < HEAD
    early = lax.rem(lane, HEAD) < HEAD // 2
    for j in range(2):
        qa = q[:, j * 128:j * 128 + 128]
        rot = jnp.where(early, -pltpu.roll(qa, 96, 1), pltpu.roll(qa, 32, 1))
        qa = qa * cos_q + rot * sin_q
        swap = pltpu.roll(qa, HEAD, 1)
        qdup[2 * j] = jnp.where(low, qa, swap).astype(bf16)
        qdup[2 * j + 1] = jnp.where(low, swap, qa).astype(bf16)

    def update(p, j):
        i = 2 * j + p
        lane_l = iota((HEAD, LMAX), 1)
        fresh = knv[i]
        for s in range(STEP):
            here = lane_l == len_s[i * STEP + s]
            rows = pl.ds(s * HEAD, HEAD)
            kcol = jnp.broadcast_to(fresh[:HEAD, s:s + 1], (HEAD, LMAX)).astype(bf16)
            vcol = jnp.broadcast_to(fresh[HEAD:, s:s + 1], (HEAD, LMAX)).astype(bf16)
            kbuf[p][j, rows, :] = jnp.where(here, kcol, kbuf[p][j, rows, :])
            vbuf[p][j, rows, :] = jnp.where(here, vcol, vbuf[p][j, rows, :])

    def attend(p, j):
        seqs = pl.ds(pl.multiple_of((2 * j + p) * STEP, STEP), STEP)
        diag = iota((STEP, BLK), 1) // HEAD == iota((STEP, BLK), 0)
        lhs = jnp.concatenate(
            [jnp.where(diag, jnp.concatenate([qdup[h, seqs, :]] * 8, axis=1), jnp.zeros((), bf16)) for h in range(4)], axis=0)
        scores = jnp.dot(lhs, kbuf[p][j], preferred_element_type=f32) * (HEAD ** -0.5)
        limit = jnp.concatenate([lenc[seqs, :]] * 4, axis=0)
        limit = jnp.concatenate([limit] * 4, axis=1)
        scores = jnp.where(iota((4 * STEP, LMAX), 1).astype(f32) <= limit, scores, -jnp.inf)
        top = jnp.max(scores, axis=-1, keepdims=True)
        expd = jnp.exp(scores - top)
        probs = (expd / jnp.sum(expd, axis=-1, keepdims=True)).astype(bf16)
        out = lax.dot_general(probs, vbuf[p][j], NT, preferred_element_type=f32)
        row_s = lax.rem(iota((4 * STEP, 128), 0), STEP)
        lane_s = iota((4 * STEP, 128), 1) // HEAD
        acc = jnp.zeros((4 * STEP, 128), f32)
        for t in range(8):
            acc = acc + jnp.where(row_s == lane_s + 2 * t, out[:, t * 128:t * 128 + 128], 0.0)
        acc = acc + pltpu.roll(acc, HEAD, 1)
        low16 = iota((STEP, 128), 1) < HEAD
        attn[seqs, :] = jnp.concatenate(
            [jnp.where(low16, acc[2 * t * STEP:(2 * t + 1) * STEP], acc[(2 * t + 1) * STEP:(2 * t + 2) * STEP]) for t in range(2)],
            axis=1).astype(bf16)

    wait(reads(0, 0))
    with scope("update"):
        update(0, 0)

    @pl.loop(0, NPAIR - 1)
    def _(j):
        with scope("kvwait"):
            wait(reads(1, j))
        with scope("pair"):
            update(1, j)
            attend(0, j)
        with scope("kvwait"):
            wait(reads(0, j + 1))
        with scope("pair"):
            update(0, j + 1)
            attend(1, j)

        @pl.when(j == HOLD)
        def _():
            for jj in range(HOLD + 1):
                start(writes(0, jj))
                start(writes(1, jj))

        @pl.when(j > HOLD)
        def _():
            start(writes(0, j))
            start(writes(1, j))

    wait(reads(1, NPAIR - 1))
    with scope("pair"):
        update(1, NPAIR - 1)
        start(writes(0, NPAIR - 1))
        start(writes(1, NPAIR - 1))
        attend(0, NPAIR - 1)
        attend(1, NPAIR - 1)

    wo_copy.wait()
    for d in range(8):
        prod = jnp.dot(attn[...], wo_v[:, d * COL:(d + 1) * COL], preferred_element_type=f32)
        part_ref[d % 2, d // 2] = prod.astype(bf16)
    with scope("drain"):
        for j in range(NPAIR):
            wait(writes(0, j))
            wait(writes(1, j))


def attn_call(lens, x, k, v, g, wq, bq, wk, bk, wv, bv, wo):
    anyspec = pl.BlockSpec(memory_space=pl.ANY)
    cache = jax.ShapeDtypeStruct((BATCH * HEAD, LMAX), bf16)
    return pl.pallas_call(
        attn_kernel,
        out_shape=(cache, cache, pltpu.VMEM((2, 4, BATCH, COL), bf16)),
        in_specs=[pl.BlockSpec(memory_space=pltpu.SMEM)] + [anyspec] * 12,
        out_specs=(anyspec, anyspec, pl.BlockSpec(memory_space=pltpu.VMEM)),
        scratch_shapes=[
            pltpu.VMEM((BATCH, D), bf16), pltpu.VMEM((1, BATCH), jnp.int32), pltpu.VMEM((16, 128), bf16),
            pltpu.VMEM((D, 4 * HEAD), bf16), pltpu.VMEM((2, 128), bf16), pltpu.VMEM((2 * HEAD, D), bf16),
            pltpu.VMEM((1, HEAD), bf16), pltpu.VMEM((1, HEAD), bf16), pltpu.VMEM((4 * HEAD, D), bf16),
            *[pltpu.VMEM((NPAIR, BLK, LMAX), bf16)] * 4,
            pltpu.VMEM((BATCH, D), bf16), pltpu.VMEM((NSTEP, 128, 128), f32), pltpu.VMEM((4, BATCH, 128), bf16),
            pltpu.VMEM((BATCH, 128), f32), pltpu.VMEM((BATCH, 4 * HEAD), bf16),
            pltpu.SemaphoreType.DMA((10,)), pltpu.SemaphoreType.DMA((4, NPAIR)), pltpu.SemaphoreType.DMA((4, NPAIR)),
        ],
        compiler_params=pltpu.CompilerParams(vmem_limit_bytes=56 * 2**20),
        cost_estimate=pl.CostEstimate(flops=10**10, bytes_accessed=70 * 2**20, transcendentals=10**6),
        name="attn",
    )(lens, x, lens.reshape(1, BATCH), k, v, g, wq, bq, wk, bk, wv, bv, wo)


def meet(me):
    barrier = pltpu.get_barrier_semaphore()
    for k in range(1, 8):
        pl.semaphore_signal(barrier, inc=1, device_id={"tp": lax.rem(me + k, 8)}, device_id_type=MESH)
    pl.semaphore_wait(barrier, 7)


def tail_kernel(part_ref, x_hbm, tok_ref, gm_ref, gf_ref, wg_hbm, wu_hbm, wd_hbm, wh_hbm,
                y_ref, out_ref,
                xown, wg_v, wu_v, wd_v, ring, part2, rs1, s2s, s2r, own, afull, yfull, mbuf, hid, fbuf, fturn, zbuf, stats, allst,
                in_sem, ring_sem, send_sem, recv_sem, st_send, st_recv):
    me = lax.axis_index("tp")
    core = lax.rem(me, 2)
    chip = me // 2
    partner = me + 1 - 2 * core
    chip_x = chip + 1 - 2 * lax.rem(chip, 2)
    chip_y = chip + 2 - 4 * (chip // 2)
    chip_d = 3 - chip

    def load(src, dst, n):
        copy = pltpu.make_async_copy(src, dst, in_sem.at[n])
        copy.start()
        return copy

    cols = pl.ds(pl.multiple_of(me * COL, COL), COL)
    xown_copy = load(x_hbm.at[:, cols], xown, 0)
    wg_copy = load(wg_hbm, wg_v, 1)
    wu_copy = load(wu_hbm, wu_v, 2)
    wd_copy = load(wd_hbm, wd_v, 3)

    def chunk(i):
        slot = lax.rem(i, NRING)
        return pltpu.make_async_copy(wh_hbm.at[pl.ds(i * VCH, VCH)], ring.at[slot], ring_sem.at[slot])

    tail_slot = NFULL % NRING
    tail_copy = pltpu.make_async_copy(wh_hbm.at[pl.ds(NFULL * VCH, VTAIL)], ring.at[tail_slot, pl.ds(0, VTAIL)],
                                      ring_sem.at[tail_slot])
    for i in range(NRING):
        chunk(i).start()

    with jax.named_scope('barrier'):
        meet(me)

    def remote(src, dst, n, dev):
        return pltpu.make_async_remote_copy(src_ref=src, dst_ref=dst, send_sem=send_sem.at[n], recv_sem=recv_sem.at[n],
                                            device_id={"tp": dev}, device_id_type=MESH)

    others = (chip_x, chip_y, chip_d)

    class Reduce:
        def __init__(self, which, half, part, full):
            self.base = (which * 2 + half) * NMSG
            self.which, self.half, self.part, self.full = which, half, part, full
            self.rows = pl.ds(half * HALF, HALF)

        def s1(self):
            return remote(self.part.at[1 - core, :, self.rows, :], rs1.at[self.which, self.half], self.base, partner)

        def s2(self, k):
            return remote(s2s.at[self.which, self.half, k], s2r.at[self.which, self.half, k], self.base + 1 + k,
                          2 * others[k] + core)

        def s3(self, k):
            block = self.full.at[me, self.rows]
            return remote(block, block, self.base + 4 + k, 2 * others[k] + core)

        def s3own(self):
            block = self.full.at[me, self.rows]
            return remote(block, block, self.base + 7, partner)

        def s4(self, k):
            block = self.full.at[2 * others[k] + core, self.rows]
            return remote(block, block, self.base + 8 + k, partner)

        @jax.named_scope('scatter')
        def scatter(self):
            self.s1().wait_recv()
            for k in (2, 0, 1):
                total = self.part[core, others[k], self.rows, :].astype(f32) + rs1[self.which, self.half, others[k]].astype(f32)
                s2s[self.which, self.half, k] = total.astype(bf16)
                self.s2(k).start()
            own[self.which, self.half] = (self.part[core, chip, self.rows, :].astype(f32)
                                          + rs1[self.which, self.half, chip].astype(f32))

        @jax.named_scope('gather')
        def gather(self, resid):
            for k in range(3):
                self.s2(k).wait_recv()
            total = resid + own[self.which, self.half]
            for k in range(3):
                total = total + s2r[self.which, self.half, k].astype(f32)
            self.full[me, self.rows, :] = total.astype(bf16)
            for k in (2, 0, 1):
                self.s3(k).start()
            self.s3own().start()

        @jax.named_scope('forward')
        def forward(self):
            for k in range(3):
                self.s3(k).wait_recv()
                self.s4(k).start()

        @jax.named_scope('finish')
        def finish(self):
            self.s3own().wait_recv()
            for k in range(3):
                self.s4(k).wait_recv()

        def drain_scatter(self):
            self.s1().wait_send()
            for k in range(3):
                self.s2(k).wait_send()

        def drain_gather(self):
            self.s3own().wait_send()
            for k in range(3):
                self.s3(k).wait_send()
                self.s4(k).wait_send()

    first = [Reduce(0, h, part_ref, afull) for h in range(2)]
    second = [Reduce(1, h, part2, yfull) for h in range(2)]

    @jax.named_scope('norm_rows')
    def norm_rows(full, half, gain_ref, dst, copy_to=None):
        @pl.loop(0, HALF // 32)
        def _(r):
            rows = pl.ds(pl.multiple_of(half * HALF + r * 32, 32), 32)
            xs = []
            for d in range(16):
                block = full[d // 2, rows, (d % 2) * 128:(d % 2) * 128 + 128]
                if copy_to is not None:
                    copy_to[rows, d * 128:(d + 1) * 128] = block
                xs.append(block.astype(f32))
            inv = inverse_rms(xs)
            for d in range(16):
                dst[rows, d * 128:(d + 1) * 128] = (xs[d] * inv * row_of(gain_ref, d, 1)).astype(bf16)

    @jax.named_scope('gate_up')
    def gate_up(half, between):
        rows = pl.ds(half * HALF, HALF)
        for n in range(4):
            if n in between:
                between[n]()
            cs = slice(n * 256, (n + 1) * 256)
            gate = jnp.dot(mbuf[rows, :], wg_v[:, cs], preferred_element_type=f32)
            up = jnp.dot(mbuf[rows, :], wu_v[:, cs], preferred_element_type=f32)
            hid[rows, cs] = (gate / (1.0 + jnp.exp(-gate)) * up).astype(bf16)

    @jax.named_scope('down')
    def down(half, after):
        rows = pl.ds(half * HALF, HALF)

        def product(c, q):
            d = (2 * q + c) * COL
            return jnp.dot(hid[rows, :], wd_v[:, pl.ds(pl.multiple_of(d, COL), COL)], preferred_element_type=f32).astype(bf16)

        for q in range(4):
            part2[1 - core, q, rows, :] = product(1 - core, q)
        after.s1().start()
        for q in range(4):
            part2[core, q, rows, :] = product(core, q)

    for h in range(2):
        first[h].s1().start()
    for h in range(2):
        first[h].scatter()
    xown_copy.wait()
    for h in range(2):
        first[h].gather(xown[h * HALF:(h + 1) * HALF, :].astype(f32))
    first[0].forward()
    first[0].finish()
    norm_rows(afull, 0, gm_ref, mbuf)
    wg_copy.wait()
    wu_copy.wait()
    gate_up(0, {3: first[1].forward})
    wd_copy.wait()
    down(0, second[0])
    for h in range(2):
        first[h].drain_scatter()
    first[1].finish()
    norm_rows(afull, 1, gm_ref, mbuf)
    gate_up(1, {AT: second[0].scatter})
    down(1, second[1])
    second[1].scatter()
    for h in range(2):
        second[h].gather(afull[me, h * HALF:(h + 1) * HALF, :].astype(f32))
    for h in range(2):
        first[h].drain_gather()
        second[h].drain_scatter()
    for h in range(2):
        second[h].forward()
        second[h].finish()
        norm_rows(yfull, h, gf_ref, fbuf, y_ref)
        with jax.named_scope("turn"):
            for d in range(8):
                cs = slice(d * COL, (d + 1) * COL)
                fturn[cs, h * HALF:(h + 1) * HALF] = fbuf[h * HALF:(h + 1) * HALF, cs].T

    tok = jnp.broadcast_to(tok_ref[...] - me * VOC, (8, BATCH))

    def absorb(buf, size, base, state):
        top, total, target = state
        z = zbuf[buf, pl.ds(0, size), :].reshape(size // 8, 8, BATCH)
        new_top = jnp.maximum(top, jnp.max(z, axis=0))
        total = total * jnp.exp(top - new_top) + jnp.sum(jnp.exp(z - new_top[None]), axis=0)
        hit = iota(z.shape, 0) * 8 + iota(z.shape, 1) == (tok - base)[None]
        target = target + jnp.sum(jnp.where(hit, z, 0.0), axis=0)
        return new_top, total, target

    def score(slot, size, base, state, before):
        for n, start in enumerate(range(0, size, SUB)):
            rows = min(SUB, size - start)
            z = jnp.dot(ring[slot, pl.ds(start, rows), :], fturn[...], preferred_element_type=f32)
            state = absorb((n + 1) % 2, SUB, before if n == 0 else base + start - SUB, state)
            zbuf[n % 2, pl.ds(0, rows), :] = z
        return state

    def head_step(t, state):
        with jax.named_scope('hwait'):
            for u in range(GROUP):
                chunk(t * GROUP + u).wait()
        for u in range(GROUP):
            i = t * GROUP + u
            before = jnp.where(i == 0, -2 * BATCH * VOC, i * VCH - SUB)
            state = score(lax.rem(i, NRING), VCH, i * VCH, state, before)
        for u in range(GROUP):
            nxt = t * GROUP + u + NRING

            @pl.when(nxt < NFULL)
            def _():
                chunk(nxt).start()

            @pl.when(nxt == NFULL)
            def _():
                tail_copy.start()
        return state

    zero = jnp.zeros((8, BATCH), f32)
    zbuf[1] = jnp.full((SUB, BATCH), -jnp.inf, f32)
    state = (jnp.full((8, BATCH), jnp.finfo(jnp.float32).min, f32), zero, zero)
    state = lax.fori_loop(0, NFULL // GROUP, head_step, state)
    tail_copy.wait()
    state = score(tail_slot, VTAIL, NFULL * VCH, state, NFULL * VCH - SUB)
    last = (VTAIL - 1) // SUB
    top8, total8, target8 = absorb(last % 2, VTAIL - last * SUB, NFULL * VCH + last * SUB, state)
    top = jnp.max(top8, axis=0, keepdims=True)
    total = jnp.sum(total8 * jnp.exp(top8 - top), axis=0, keepdims=True)
    target = jnp.sum(target8, axis=0, keepdims=True)
    zero = jnp.zeros((1, BATCH), f32)

    stats[...] = jnp.concatenate([top, total, target, zero, zero, zero, zero, zero], axis=0)
    allst[me] = stats[...]

    def stat_copy(k):
        return pltpu.make_async_remote_copy(src_ref=stats, dst_ref=allst.at[me], send_sem=st_send.at[k - 1],
                                            recv_sem=st_recv.at[k - 1], device_id={"tp": lax.rem(me + k, 8)},
                                            device_id_type=MESH)

    for k in range(1, 8):
        stat_copy(k).start()
    with jax.named_scope('statwait'):
        for h in range(2):
            second[h].drain_gather()
        for k in range(1, 8):
            stat_copy(k).wait_recv()
        for k in range(1, 8):
            stat_copy(k).wait_send()
    out_ref[...] = allst[...]


def tail_call(part, x, tok, gm, gf, wg, wu, wd, wh):
    anyspec = pl.BlockSpec(memory_space=pl.ANY)
    vspec = pl.BlockSpec(memory_space=pltpu.VMEM)
    blocks = (2, 2, 3, HALF, COL)
    return pl.pallas_call(
        tail_kernel,
        out_shape=(pltpu.VMEM((BATCH, D), bf16), pltpu.VMEM((8, 8, BATCH), f32)),
        in_specs=[vspec, anyspec, vspec, vspec, vspec, anyspec, anyspec, anyspec, anyspec],
        out_specs=(vspec, vspec),
        scratch_shapes=[
            pltpu.VMEM((BATCH, COL), bf16), pltpu.VMEM((D, FF), bf16), pltpu.VMEM((D, FF), bf16), pltpu.VMEM((FF, D), bf16),
            pltpu.VMEM((NRING, VCH, D), bf16), pltpu.VMEM((2, 4, BATCH, COL), bf16), pltpu.VMEM((2, 2, 4, HALF, COL), bf16),
            pltpu.VMEM(blocks, bf16), pltpu.VMEM(blocks, bf16), pltpu.VMEM((2, 2, HALF, COL), f32),
            pltpu.VMEM((8, BATCH, COL), bf16), pltpu.VMEM((8, BATCH, COL), bf16), pltpu.VMEM((BATCH, D), bf16),
            pltpu.VMEM((BATCH, FF), bf16), pltpu.VMEM((BATCH, D), bf16), pltpu.VMEM((D, BATCH), bf16), pltpu.VMEM((2, SUB, BATCH), f32),
            pltpu.VMEM((8, BATCH), f32), pltpu.VMEM((8, 8, BATCH), f32),
            pltpu.SemaphoreType.DMA((4,)), pltpu.SemaphoreType.DMA((NRING,)), pltpu.SemaphoreType.DMA((4 * NMSG,)),
            pltpu.SemaphoreType.DMA((4 * NMSG,)), pltpu.SemaphoreType.DMA((7,)), pltpu.SemaphoreType.DMA((7,)),
        ],
        compiler_params=pltpu.CompilerParams(collective_id=0, has_side_effects=True, vmem_limit_bytes=54 * 2**20),
        cost_estimate=pl.CostEstimate(flops=2 * 10**10, bytes_accessed=80 * 2**20, transcendentals=10**6),
        name="tail",
    )(pltpu.with_memory_space_constraint(part, pltpu.VMEM), x, tok, gm, gf, wg, wu, wd, wh)


def end_kernel(y_ref, allst, y_hbm, logp_hbm, lse_hbm, rows_v, sem):
    copies = [pltpu.make_async_copy(y_ref, y_hbm, sem.at[0])]
    copies[0].start()
    top = allst[0, 0:1, :]
    for d in range(1, 8):
        top = jnp.maximum(top, allst[d, 0:1, :])
    total = jnp.zeros((1, BATCH), f32)
    target = jnp.zeros((1, BATCH), f32)
    for d in range(8):
        total = total + allst[d, 1:2, :] * jnp.exp(allst[d, 0:1, :] - top)
        target = target + allst[d, 2:3, :]
    lse = top + jnp.log(total)
    rows_v[0] = target - lse
    rows_v[1] = lse
    for n, dst in enumerate((logp_hbm, lse_hbm)):
        copies.append(pltpu.make_async_copy(rows_v.at[n], dst, sem.at[1 + n]))
        copies[-1].start()
    for copy in copies:
        copy.wait()


def end_call(y, stats):
    vspec = pl.BlockSpec(memory_space=pltpu.VMEM)
    row = jax.ShapeDtypeStruct((1, BATCH), f32)
    return pl.pallas_call(
        end_kernel,
        out_shape=(jax.ShapeDtypeStruct((BATCH, D), bf16), row, row),
        in_specs=[vspec, vspec],
        out_specs=(pl.BlockSpec(memory_space=pltpu.HBM),) * 3,
        scratch_shapes=[pltpu.VMEM((2, 1, BATCH), f32), pltpu.SemaphoreType.DMA((3,))],
        compiler_params=pltpu.CompilerParams(vmem_limit_bytes=4 * 2**20),
        name="end",
    )(y, stats)


def local_step(x, lens, k_cache, v_cache, tok, g_attn, w_q, b_q, w_k, b_k, w_v, b_v, w_o, g_mlp, w_gate, w_up, w_down, g_final, w_head):
    def flat(cache):
        return cache.transpose(0, 2, 3, 1).reshape(BATCH * HEAD, LMAX)

    def unflat(cache):
        return cache.reshape(BATCH, 1, HEAD, LMAX).transpose(0, 3, 1, 2)

    k_new, v_new, part = attn_call(lens, x, flat(k_cache), flat(v_cache), g_attn.reshape(16, 128), w_q, b_q.reshape(2, 128),
                                   w_k.T, b_k.reshape(1, -1), w_v.T, b_v.reshape(1, -1), w_o)
    y, logp, lse = end_call(*tail_call(part, x, tok.reshape(1, BATCH), g_mlp.reshape(16, 128), g_final.reshape(16, 128), w_gate, w_up, w_down, w_head))
    return y, unflat(k_new), unflat(v_new), logp.reshape(BATCH), lse.reshape(BATCH)


def solution(mesh):
    row_spec = P('dp', None)
    vec_spec = P('dp')
    cache_spec = P('dp', None, 'tp', None)
    col_spec = P(None, 'tp')
    part_spec = P('tp')
    whole_spec = P(None)
    in_specs = (row_spec, vec_spec, cache_spec, cache_spec, vec_spec, whole_spec, col_spec, part_spec, col_spec, part_spec, col_spec, part_spec, P('tp', None), whole_spec, col_spec, col_spec, P('tp', None), whole_spec, P('tp', None))
    out_specs = (row_spec, cache_spec, cache_spec, vec_spec, vec_spec)
    return jax.shard_map(local_step, mesh=mesh, in_specs=in_specs, out_specs=out_specs, check_vma=False)
```

```python
import functools
import math

import jax
import jax.numpy as jnp
from jax import lax
from jax.experimental import pallas as pl
from jax.experimental.pallas import tpu as pltpu
from jax.sharding import PartitionSpec as P

THETA = 1000000.0
EPS = 1e-6
BATCH = 256
LMAX = 512
D = 2048
HEAD = 64
FF = 1024
STEP = 16
NSTEP = BATCH // STEP
BLK = STEP * HEAD
NPAIR = NSTEP // 2
HOLD = 2
COL = D // 8
HALF = BATCH // 2
NMSG = 11
AT = 1
VOC = 16032
VCH = 1024
NFULL = VOC // VCH
VTAIL = VOC - NFULL * VCH
NRING = 7
SUB = 256
GROUP = 3

f32 = jnp.float32
bf16 = jnp.bfloat16
NT = (((1,), (1,)), ((), ()))
MESH = pl.DeviceIdType.MESH


def iota(shape, dim):
    return lax.broadcasted_iota(jnp.int32, shape, dim)


def row_of(ref, start, count):
    return jnp.concatenate([ref[start + i:start + i + 1, :] for i in range(count)], axis=1).astype(f32)


def inverse_rms(pieces):
    squares = [piece * piece for piece in pieces]
    while len(squares) > 1:
        squares = [squares[i] + squares[i + 1] for i in range(0, len(squares), 2)]
    return lax.rsqrt(jnp.sum(squares[0], axis=-1, keepdims=True) * (1.0 / D) + EPS)


def attn_kernel(len1_hbm, x_hbm, len_hbm, k_hbm, v_hbm, g_hbm, wq_hbm, bq_hbm, wk_hbm, bk_hbm, wv_hbm, bv_hbm, wo_hbm,
                ko_hbm, vo_hbm, part_ref,
                len_s, x_v, len_v, g_v, wq_v, bq_v, wkv_v, bk_v, bv_v, wo_v, kbuf0, kbuf1, vbuf0, vbuf1, normed, knv, qdup, lenc, attn,
                in_sem, rd_sem, wr_sem):
    def load(src, dst, n):
        copy = pltpu.make_async_copy(src, dst, in_sem.at[n])
        copy.start()
        return copy

    scope = jax.named_scope
    small = [
        load(x_hbm, x_v, 0),
        load(g_hbm, g_v, 1),
        load(len_hbm, len_v, 2),
        load(wk_hbm, wkv_v.at[pl.ds(0, HEAD)], 3),
        load(wv_hbm, wkv_v.at[pl.ds(HEAD, HEAD)], 4),
        load(bk_hbm, bk_v, 5),
        load(bv_hbm, bv_v, 6),
        load(wq_hbm, wq_v, 7),
        load(bq_hbm, bq_v, 8),
        load(len1_hbm, len_s, 10),
    ]

    kbuf, vbuf = (kbuf0, kbuf1), (vbuf0, vbuf1)

    def reads(p, j):
        rows = pl.ds((2 * j + p) * BLK, BLK)
        return (pltpu.make_async_copy(k_hbm.at[rows], kbuf[p].at[j], rd_sem.at[p, j]),
                pltpu.make_async_copy(v_hbm.at[rows], vbuf[p].at[j], rd_sem.at[2 + p, j]))

    def writes(p, j):
        rows = pl.ds((2 * j + p) * BLK, BLK)
        return (pltpu.make_async_copy(kbuf[p].at[j], ko_hbm.at[rows], wr_sem.at[p, j]),
                pltpu.make_async_copy(vbuf[p].at[j], vo_hbm.at[rows], wr_sem.at[2 + p, j]))

    def start(copies):
        for copy in copies:
            copy.start()

    def wait(copies):
        for copy in copies:
            copy.wait()

    start(reads(0, 0))
    start(reads(1, 0))
    with scope("loads"):
        for copy in small:
            copy.wait()
    for j in range(1, NPAIR):
        start(reads(0, j))
        start(reads(1, j))
    wo_copy = load(wo_hbm, wo_v, 9)

    @pl.loop(0, BATCH // 32)
    @scope("norm")
    def _(r):
        rows = pl.ds(pl.multiple_of(r * 32, 32), 32)
        xs = [x_v[rows, d * 128:(d + 1) * 128].astype(f32) for d in range(16)]
        inv = inverse_rms(xs)
        for d in range(16):
            normed[rows, d * 128:(d + 1) * 128] = (xs[d] * inv * row_of(g_v, d, 1)).astype(bf16)

    freq = jnp.exp(iota((HEAD // 2, BATCH), 0).astype(f32) * (-2.0 / HEAD * math.log(THETA)))
    angles = jnp.broadcast_to(len_v[...].astype(f32), (HEAD // 2, BATCH)) * freq
    cos_t = jnp.cos(angles)
    sin_t = jnp.sin(angles)
    cos_q = jnp.concatenate([cos_t] * 4, axis=0).T
    sin_q = jnp.concatenate([sin_t] * 4, axis=0).T
    lenc[...] = jnp.broadcast_to(len_v[...], (128, BATCH)).astype(f32).T

    bias = jnp.concatenate([bk_v[...].astype(f32), bv_v[...].astype(f32)], axis=1)
    bias = jnp.broadcast_to(bias, (128, 128)).T
    bias = jnp.concatenate([bias, bias], axis=1)
    kv = lax.dot_general(wkv_v[...], normed[...], NT, preferred_element_type=f32) + bias
    first, second = kv[:HEAD // 2], kv[HEAD // 2:HEAD]
    kv = jnp.concatenate([first * cos_t - second * sin_t, second * cos_t + first * sin_t, kv[HEAD:]], axis=0)
    kv = kv.astype(bf16).astype(f32)
    for i in range(NSTEP):
        part = kv[:, (i // 8) * 128:(i // 8) * 128 + 128]
        shift = (128 - STEP * (i % 8)) % 128
        knv[i] = pltpu.roll(part, shift, 1) if shift else part

    q = jnp.dot(normed[...], wq_v[...], preferred_element_type=f32) + row_of(bq_v, 0, 2)
    lane = iota((BATCH, 128), 1)
    low = lane < HEAD
    early = lax.rem(lane, HEAD) < HEAD // 2
    for j in range(2):
        qa = q[:, j * 128:j * 128 + 128]
        rot = jnp.where(early, -pltpu.roll(qa, 96, 1), pltpu.roll(qa, 32, 1))
        qa = qa * cos_q + rot * sin_q
        swap = pltpu.roll(qa, HEAD, 1)
        qdup[2 * j] = jnp.where(low, qa, swap).astype(bf16)
        qdup[2 * j + 1] = jnp.where(low, swap, qa).astype(bf16)

    def update(p, j):
        i = 2 * j + p
        lane_l = iota((HEAD, LMAX), 1)
        fresh = knv[i]
        for s in range(STEP):
            here = lane_l == len_s[i * STEP + s]
            rows = pl.ds(s * HEAD, HEAD)
            kcol = jnp.broadcast_to(fresh[:HEAD, s:s + 1], (HEAD, LMAX)).astype(bf16)
            vcol = jnp.broadcast_to(fresh[HEAD:, s:s + 1], (HEAD, LMAX)).astype(bf16)
            kbuf[p][j, rows, :] = jnp.where(here, kcol, kbuf[p][j, rows, :])
            vbuf[p][j, rows, :] = jnp.where(here, vcol, vbuf[p][j, rows, :])

    def attend(p, j):
        seqs = pl.ds(pl.multiple_of((2 * j + p) * STEP, STEP), STEP)
        diag = iota((STEP, BLK), 1) // HEAD == iota((STEP, BLK), 0)
        lhs = jnp.concatenate(
            [jnp.where(diag, jnp.concatenate([qdup[h, seqs, :]] * 8, axis=1), jnp.zeros((), bf16)) for h in range(4)], axis=0)
        scores = jnp.dot(lhs, kbuf[p][j], preferred_element_type=f32) * (HEAD ** -0.5)
        limit = jnp.concatenate([lenc[seqs, :]] * 4, axis=0)
        limit = jnp.concatenate([limit] * 4, axis=1)
        scores = jnp.where(iota((4 * STEP, LMAX), 1).astype(f32) <= limit, scores, -jnp.inf)
        top = jnp.max(scores, axis=-1, keepdims=True)
        expd = jnp.exp(scores - top)
        probs = (expd / jnp.sum(expd, axis=-1, keepdims=True)).astype(bf16)
        out = lax.dot_general(probs, vbuf[p][j], NT, preferred_element_type=f32)
        row_s = lax.rem(iota((4 * STEP, 128), 0), STEP)
        lane_s = iota((4 * STEP, 128), 1) // HEAD
        acc = jnp.zeros((4 * STEP, 128), f32)
        for t in range(8):
            acc = acc + jnp.where(row_s == lane_s + 2 * t, out[:, t * 128:t * 128 + 128], 0.0)
        acc = acc + pltpu.roll(acc, HEAD, 1)
        low16 = iota((STEP, 128), 1) < HEAD
        attn[seqs, :] = jnp.concatenate(
            [jnp.where(low16, acc[2 * t * STEP:(2 * t + 1) * STEP], acc[(2 * t + 1) * STEP:(2 * t + 2) * STEP]) for t in range(2)],
            axis=1).astype(bf16)

    wait(reads(0, 0))
    with scope("update"):
        update(0, 0)

    @pl.loop(0, NPAIR - 1)
    def _(j):
        with scope("kvwait"):
            wait(reads(1, j))
        with scope("pair"):
            update(1, j)
            attend(0, j)
        with scope("kvwait"):
            wait(reads(0, j + 1))
        with scope("pair"):
            update(0, j + 1)
            attend(1, j)

        @pl.when(j == HOLD)
        def _():
            for jj in range(HOLD + 1):
                start(writes(0, jj))
                start(writes(1, jj))

        @pl.when(j > HOLD)
        def _():
            start(writes(0, j))
            start(writes(1, j))

    wait(reads(1, NPAIR - 1))
    with scope("pair"):
        update(1, NPAIR - 1)
        start(writes(0, NPAIR - 1))
        start(writes(1, NPAIR - 1))
        attend(0, NPAIR - 1)
        attend(1, NPAIR - 1)

    wo_copy.wait()
    for d in range(8):
        prod = jnp.dot(attn[...], wo_v[:, d * COL:(d + 1) * COL], preferred_element_type=f32)
        part_ref[d % 2, d // 2] = prod.astype(bf16)
    with scope("drain"):
        for j in range(NPAIR):
            wait(writes(0, j))
            wait(writes(1, j))


def attn_call(lens, x, k, v, g, wq, bq, wk, bk, wv, bv, wo):
    anyspec = pl.BlockSpec(memory_space=pl.ANY)
    cache = jax.ShapeDtypeStruct((BATCH * HEAD, LMAX), bf16)
    return pl.pallas_call(
        attn_kernel,
        out_shape=(cache, cache, pltpu.VMEM((2, 4, BATCH, COL), bf16)),
        in_specs=[anyspec] * 13,
        out_specs=(anyspec, anyspec, pl.BlockSpec(memory_space=pltpu.VMEM)),
        scratch_shapes=[
            pltpu.SMEM((BATCH,), jnp.int32),
            pltpu.VMEM((BATCH, D), bf16), pltpu.VMEM((1, BATCH), jnp.int32), pltpu.VMEM((16, 128), bf16),
            pltpu.VMEM((D, 4 * HEAD), bf16), pltpu.VMEM((2, 128), bf16), pltpu.VMEM((2 * HEAD, D), bf16),
            pltpu.VMEM((1, HEAD), bf16), pltpu.VMEM((1, HEAD), bf16), pltpu.VMEM((4 * HEAD, D), bf16),
            *[pltpu.VMEM((NPAIR, BLK, LMAX), bf16)] * 4,
            pltpu.VMEM((BATCH, D), bf16), pltpu.VMEM((NSTEP, 128, 128), f32), pltpu.VMEM((4, BATCH, 128), bf16),
            pltpu.VMEM((BATCH, 128), f32), pltpu.VMEM((BATCH, 4 * HEAD), bf16),
            pltpu.SemaphoreType.DMA((11,)), pltpu.SemaphoreType.DMA((4, NPAIR)), pltpu.SemaphoreType.DMA((4, NPAIR)),
        ],
        compiler_params=pltpu.CompilerParams(vmem_limit_bytes=56 * 2**20),
        cost_estimate=pl.CostEstimate(flops=10**10, bytes_accessed=70 * 2**20, transcendentals=10**6),
        name="attn",
    )(lens, x, lens.reshape(1, BATCH), k, v, g, wq, bq, wk, bk, wv, bv, wo)


def meet(me):
    barrier = pltpu.get_barrier_semaphore()
    for k in range(1, 8):
        pl.semaphore_signal(barrier, inc=1, device_id={"tp": lax.rem(me + k, 8)}, device_id_type=MESH)
    pl.semaphore_wait(barrier, 7)


def tail_kernel(part_ref, x_hbm, tok_hbm, gm_hbm, gf_hbm, wg_hbm, wu_hbm, wd_hbm, wh_hbm,
                y_ref, out_ref,
                tok_ref, gm_ref, gf_ref, xown, wg_v, wu_v, wd_v, ring, part2, rs1, s2s, s2r, own, afull, yfull, mbuf, hid, fbuf, fturn, zbuf, stats, allst,
                in_sem, ring_sem, send_sem, recv_sem, st_send, st_recv):
    me = lax.axis_index("tp")
    core = lax.rem(me, 2)
    chip = me // 2
    partner = me + 1 - 2 * core
    chip_x = chip + 1 - 2 * lax.rem(chip, 2)
    chip_y = chip + 2 - 4 * (chip // 2)
    chip_d = 3 - chip

    def load(src, dst, n):
        copy = pltpu.make_async_copy(src, dst, in_sem.at[n])
        copy.start()
        return copy

    cols = pl.ds(pl.multiple_of(me * COL, COL), COL)
    xown_copy = load(x_hbm.at[:, cols], xown, 0)
    gains = [load(gm_hbm, gm_ref, 4), load(gf_hbm, gf_ref, 5), load(tok_hbm, tok_ref, 6)]
    wg_copy = load(wg_hbm, wg_v, 1)
    wu_copy = load(wu_hbm, wu_v, 2)
    wd_copy = load(wd_hbm, wd_v, 3)

    def chunk(i):
        slot = lax.rem(i, NRING)
        return pltpu.make_async_copy(wh_hbm.at[pl.ds(i * VCH, VCH)], ring.at[slot], ring_sem.at[slot])

    tail_slot = NFULL % NRING
    tail_copy = pltpu.make_async_copy(wh_hbm.at[pl.ds(NFULL * VCH, VTAIL)], ring.at[tail_slot, pl.ds(0, VTAIL)],
                                      ring_sem.at[tail_slot])
    for i in range(NRING):
        chunk(i).start()

    with jax.named_scope('barrier'):
        meet(me)

    def remote(src, dst, n, dev):
        return pltpu.make_async_remote_copy(src_ref=src, dst_ref=dst, send_sem=send_sem.at[n], recv_sem=recv_sem.at[n],
                                            device_id={"tp": dev}, device_id_type=MESH)

    others = (chip_x, chip_y, chip_d)

    class Reduce:
        def __init__(self, which, half, part, full):
            self.base = (which * 2 + half) * NMSG
            self.which, self.half, self.part, self.full = which, half, part, full
            self.rows = pl.ds(half * HALF, HALF)

        def s1(self):
            return remote(self.part.at[1 - core, :, self.rows, :], rs1.at[self.which, self.half], self.base, partner)

        def s2(self, k):
            return remote(s2s.at[self.which, self.half, k], s2r.at[self.which, self.half, k], self.base + 1 + k,
                          2 * others[k] + core)

        def s3(self, k):
            block = self.full.at[me, self.rows]
            return remote(block, block, self.base + 4 + k, 2 * others[k] + core)

        def s3own(self):
            block = self.full.at[me, self.rows]
            return remote(block, block, self.base + 7, partner)

        def s4(self, k):
            block = self.full.at[2 * others[k] + core, self.rows]
            return remote(block, block, self.base + 8 + k, partner)

        @jax.named_scope('scatter')
        def scatter(self):
            self.s1().wait_recv()
            for k in (2, 0, 1):
                total = self.part[core, others[k], self.rows, :].astype(f32) + rs1[self.which, self.half, others[k]].astype(f32)
                s2s[self.which, self.half, k] = total.astype(bf16)
                self.s2(k).start()
            own[self.which, self.half] = (self.part[core, chip, self.rows, :].astype(f32)
                                          + rs1[self.which, self.half, chip].astype(f32))

        @jax.named_scope('gather')
        def gather(self, resid):
            for k in range(3):
                self.s2(k).wait_recv()
            total = resid + own[self.which, self.half]
            for k in range(3):
                total = total + s2r[self.which, self.half, k].astype(f32)
            self.full[me, self.rows, :] = total.astype(bf16)
            for k in (2, 0, 1):
                self.s3(k).start()
            self.s3own().start()

        @jax.named_scope('forward')
        def forward(self):
            for k in range(3):
                self.s3(k).wait_recv()
                self.s4(k).start()

        @jax.named_scope('finish')
        def finish(self):
            self.s3own().wait_recv()
            for k in range(3):
                self.s4(k).wait_recv()

        def drain_scatter(self):
            self.s1().wait_send()
            for k in range(3):
                self.s2(k).wait_send()

        def drain_gather(self):
            self.s3own().wait_send()
            for k in range(3):
                self.s3(k).wait_send()
                self.s4(k).wait_send()

    first = [Reduce(0, h, part_ref, afull) for h in range(2)]
    second = [Reduce(1, h, part2, yfull) for h in range(2)]

    @jax.named_scope('norm_rows')
    def norm_rows(full, half, gain_ref, dst, copy_to=None):
        @pl.loop(0, HALF // 32)
        def _(r):
            rows = pl.ds(pl.multiple_of(half * HALF + r * 32, 32), 32)
            xs = []
            for d in range(16):
                block = full[d // 2, rows, (d % 2) * 128:(d % 2) * 128 + 128]
                if copy_to is not None:
                    copy_to[rows, d * 128:(d + 1) * 128] = block
                xs.append(block.astype(f32))
            inv = inverse_rms(xs)
            for d in range(16):
                dst[rows, d * 128:(d + 1) * 128] = (xs[d] * inv * row_of(gain_ref, d, 1)).astype(bf16)

    @jax.named_scope('gate_up')
    def gate_up(half, between):
        rows = pl.ds(half * HALF, HALF)
        for n in range(4):
            if n in between:
                between[n]()
            cs = slice(n * 256, (n + 1) * 256)
            gate = jnp.dot(mbuf[rows, :], wg_v[:, cs], preferred_element_type=f32)
            up = jnp.dot(mbuf[rows, :], wu_v[:, cs], preferred_element_type=f32)
            hid[rows, cs] = (gate / (1.0 + jnp.exp(-gate)) * up).astype(bf16)

    @jax.named_scope('down')
    def down(half, after):
        rows = pl.ds(half * HALF, HALF)

        def product(c, q):
            d = (2 * q + c) * COL
            return jnp.dot(hid[rows, :], wd_v[:, pl.ds(pl.multiple_of(d, COL), COL)], preferred_element_type=f32).astype(bf16)

        for q in range(4):
            part2[1 - core, q, rows, :] = product(1 - core, q)
        after.s1().start()
        for q in range(4):
            part2[core, q, rows, :] = product(core, q)

    for h in range(2):
        first[h].s1().start()
    for h in range(2):
        first[h].scatter()
    xown_copy.wait()
    for copy in gains:
        copy.wait()
    for h in range(2):
        first[h].gather(xown[h * HALF:(h + 1) * HALF, :].astype(f32))
    first[0].forward()
    first[0].finish()
    norm_rows(afull, 0, gm_ref, mbuf)
    wg_copy.wait()
    wu_copy.wait()
    gate_up(0, {3: first[1].forward})
    wd_copy.wait()
    down(0, second[0])
    for h in range(2):
        first[h].drain_scatter()
    first[1].finish()
    norm_rows(afull, 1, gm_ref, mbuf)
    gate_up(1, {AT: second[0].scatter})
    down(1, second[1])
    second[1].scatter()
    for h in range(2):
        second[h].gather(afull[me, h * HALF:(h + 1) * HALF, :].astype(f32))
    for h in range(2):
        first[h].drain_gather()
        second[h].drain_scatter()
    for h in range(2):
        second[h].forward()
        second[h].finish()
        norm_rows(yfull, h, gf_ref, fbuf, y_ref)
        with jax.named_scope("turn"):
            for d in range(8):
                cs = slice(d * COL, (d + 1) * COL)
                fturn[cs, h * HALF:(h + 1) * HALF] = fbuf[h * HALF:(h + 1) * HALF, cs].T

    tok = jnp.broadcast_to(tok_ref[...] - me * VOC, (8, BATCH))

    def absorb(buf, size, base, state):
        top, total, target = state
        z = zbuf[buf, pl.ds(0, size), :].reshape(size // 8, 8, BATCH)
        new_top = jnp.maximum(top, jnp.max(z, axis=0))
        total = total * jnp.exp(top - new_top) + jnp.sum(jnp.exp(z - new_top[None]), axis=0)
        hit = iota(z.shape, 0) * 8 + iota(z.shape, 1) == (tok - base)[None]
        target = target + jnp.sum(jnp.where(hit, z, 0.0), axis=0)
        return new_top, total, target

    def score(slot, size, base, state, before):
        for n, start in enumerate(range(0, size, SUB)):
            rows = min(SUB, size - start)
            z = jnp.dot(ring[slot, pl.ds(start, rows), :], fturn[...], preferred_element_type=f32)
            state = absorb((n + 1) % 2, SUB, before if n == 0 else base + start - SUB, state)
            zbuf[n % 2, pl.ds(0, rows), :] = z
        return state

    def head_step(t, state):
        with jax.named_scope('hwait'):
            for u in range(GROUP):
                chunk(t * GROUP + u).wait()
        for u in range(GROUP):
            i = t * GROUP + u
            before = jnp.where(i == 0, -2 * BATCH * VOC, i * VCH - SUB)
            state = score(lax.rem(i, NRING), VCH, i * VCH, state, before)
        for u in range(GROUP):
            nxt = t * GROUP + u + NRING

            @pl.when(nxt < NFULL)
            def _():
                chunk(nxt).start()

            @pl.when(nxt == NFULL)
            def _():
                tail_copy.start()
        return state

    zero = jnp.zeros((8, BATCH), f32)
    zbuf[1] = jnp.full((SUB, BATCH), -jnp.inf, f32)
    state = (jnp.full((8, BATCH), jnp.finfo(jnp.float32).min, f32), zero, zero)
    state = lax.fori_loop(0, NFULL // GROUP, head_step, state)
    tail_copy.wait()
    state = score(tail_slot, VTAIL, NFULL * VCH, state, NFULL * VCH - SUB)
    last = (VTAIL - 1) // SUB
    top8, total8, target8 = absorb(last % 2, VTAIL - last * SUB, NFULL * VCH + last * SUB, state)
    top = jnp.max(top8, axis=0, keepdims=True)
    total = jnp.sum(total8 * jnp.exp(top8 - top), axis=0, keepdims=True)
    target = jnp.sum(target8, axis=0, keepdims=True)
    zero = jnp.zeros((1, BATCH), f32)

    stats[...] = jnp.concatenate([top, total, target, zero, zero, zero, zero, zero], axis=0)
    allst[me] = stats[...]

    def stat_copy(k):
        return pltpu.make_async_remote_copy(src_ref=stats, dst_ref=allst.at[me], send_sem=st_send.at[k - 1],
                                            recv_sem=st_recv.at[k - 1], device_id={"tp": lax.rem(me + k, 8)},
                                            device_id_type=MESH)

    for k in range(1, 8):
        stat_copy(k).start()
    with jax.named_scope('statwait'):
        for h in range(2):
            second[h].drain_gather()
        for k in range(1, 8):
            stat_copy(k).wait_recv()
        for k in range(1, 8):
            stat_copy(k).wait_send()
    out_ref[...] = allst[...]


def tail_call(part, x, tok, gm, gf, wg, wu, wd, wh):
    anyspec = pl.BlockSpec(memory_space=pl.ANY)
    vspec = pl.BlockSpec(memory_space=pltpu.VMEM)
    blocks = (2, 2, 3, HALF, COL)
    return pl.pallas_call(
        tail_kernel,
        out_shape=(pltpu.VMEM((BATCH, D), bf16), pltpu.VMEM((8, 8, BATCH), f32)),
        in_specs=[vspec] + [anyspec] * 8,
        out_specs=(vspec, vspec),
        scratch_shapes=[
            pltpu.VMEM((1, BATCH), jnp.int32), pltpu.VMEM((16, 128), bf16), pltpu.VMEM((16, 128), bf16),
            pltpu.VMEM((BATCH, COL), bf16), pltpu.VMEM((D, FF), bf16), pltpu.VMEM((D, FF), bf16), pltpu.VMEM((FF, D), bf16),
            pltpu.VMEM((NRING, VCH, D), bf16), pltpu.VMEM((2, 4, BATCH, COL), bf16), pltpu.VMEM((2, 2, 4, HALF, COL), bf16),
            pltpu.VMEM(blocks, bf16), pltpu.VMEM(blocks, bf16), pltpu.VMEM((2, 2, HALF, COL), f32),
            pltpu.VMEM((8, BATCH, COL), bf16), pltpu.VMEM((8, BATCH, COL), bf16), pltpu.VMEM((BATCH, D), bf16),
            pltpu.VMEM((BATCH, FF), bf16), pltpu.VMEM((BATCH, D), bf16), pltpu.VMEM((D, BATCH), bf16), pltpu.VMEM((2, SUB, BATCH), f32),
            pltpu.VMEM((8, BATCH), f32), pltpu.VMEM((8, 8, BATCH), f32),
            pltpu.SemaphoreType.DMA((7,)), pltpu.SemaphoreType.DMA((NRING,)), pltpu.SemaphoreType.DMA((4 * NMSG,)),
            pltpu.SemaphoreType.DMA((4 * NMSG,)), pltpu.SemaphoreType.DMA((7,)), pltpu.SemaphoreType.DMA((7,)),
        ],
        compiler_params=pltpu.CompilerParams(collective_id=0, has_side_effects=True, vmem_limit_bytes=54 * 2**20),
        cost_estimate=pl.CostEstimate(flops=2 * 10**10, bytes_accessed=80 * 2**20, transcendentals=10**6),
        name="tail",
    )(pltpu.with_memory_space_constraint(part, pltpu.VMEM), x, tok, gm, gf, wg, wu, wd, wh)


def end_kernel(y_ref, allst, y_hbm, logp_hbm, lse_hbm, rows_v, sem):
    copies = [pltpu.make_async_copy(y_ref, y_hbm, sem.at[0])]
    copies[0].start()
    top = allst[0, 0:1, :]
    for d in range(1, 8):
        top = jnp.maximum(top, allst[d, 0:1, :])
    total = jnp.zeros((1, BATCH), f32)
    target = jnp.zeros((1, BATCH), f32)
    for d in range(8):
        total = total + allst[d, 1:2, :] * jnp.exp(allst[d, 0:1, :] - top)
        target = target + allst[d, 2:3, :]
    lse = top + jnp.log(total)
    rows_v[0] = target - lse
    rows_v[1] = lse
    for n, dst in enumerate((logp_hbm, lse_hbm)):
        copies.append(pltpu.make_async_copy(rows_v.at[n], dst, sem.at[1 + n]))
        copies[-1].start()
    for copy in copies:
        copy.wait()


def end_call(y, stats):
    vspec = pl.BlockSpec(memory_space=pltpu.VMEM)
    row = jax.ShapeDtypeStruct((1, BATCH), f32)
    return pl.pallas_call(
        end_kernel,
        out_shape=(jax.ShapeDtypeStruct((BATCH, D), bf16), row, row),
        in_specs=[vspec, vspec],
        out_specs=(pl.BlockSpec(memory_space=pltpu.HBM),) * 3,
        scratch_shapes=[pltpu.VMEM((2, 1, BATCH), f32), pltpu.SemaphoreType.DMA((3,))],
        compiler_params=pltpu.CompilerParams(vmem_limit_bytes=4 * 2**20),
        name="end",
    )(y, stats)


def local_step(x, lens, k_cache, v_cache, tok, g_attn, w_q, b_q, w_k, b_k, w_v, b_v, w_o, g_mlp, w_gate, w_up, w_down, g_final, w_head):
    def flat(cache):
        return cache.transpose(0, 2, 3, 1).reshape(BATCH * HEAD, LMAX)

    def unflat(cache):
        return cache.reshape(BATCH, 1, HEAD, LMAX).transpose(0, 3, 1, 2)

    k_new, v_new, part = attn_call(lens, x, flat(k_cache), flat(v_cache), g_attn.reshape(16, 128), w_q, b_q.reshape(2, 128),
                                   w_k.T, b_k.reshape(1, -1), w_v.T, b_v.reshape(1, -1), w_o)
    y, logp, lse = end_call(*tail_call(part, x, tok.reshape(1, BATCH), g_mlp.reshape(16, 128), g_final.reshape(16, 128), w_gate, w_up, w_down, w_head))
    return y, unflat(k_new), unflat(v_new), logp.reshape(BATCH), lse.reshape(BATCH)


def solution(mesh):
    row_spec = P('dp', None)
    vec_spec = P('dp')
    cache_spec = P('dp', None, 'tp', None)
    col_spec = P(None, 'tp')
    part_spec = P('tp')
    whole_spec = P(None)
    in_specs = (row_spec, vec_spec, cache_spec, cache_spec, vec_spec, whole_spec, col_spec, part_spec, col_spec, part_spec, col_spec, part_spec, P('tp', None), whole_spec, col_spec, col_spec, P('tp', None), whole_spec, P('tp', None))
    out_specs = (row_spec, cache_spec, cache_spec, vec_spec, vec_spec)
    return jax.shard_map(local_step, mesh=mesh, in_specs=in_specs, out_specs=out_specs, check_vma=False)
```
